256 devices in a mesh: feat: 8 (over y, core), rows: 32 (over z, x).
Axes of the slice: x: 4, y: 4, z: 8, core: 2. Of those that a mesh axis runs over, the one named last changes fastest.
Arguments:
- test_cells: float32 [256, 96, 192], P('rows', 'feat'), may hold values from -12 to 12
- train_cells: float32 [16384, 96, 192], P('rows', 'feat'), may hold values from -6 to 6
- w_query: float32 [192, 192], P('feat'), may hold values from -1.5 to 1.5
- w_key: float32 [192, 192], P('feat'), may hold values from -1.5 to 1.5
- w_value: float32 [192, 192], P('feat'), may hold values from -0.4375 to 0.4375
- w_out: float32 [192, 192], P('feat'), may hold values from -0.4375 to 0.4375
Outputs:
- attended: float32 [256, 96, 192], P('rows', 'feat')
The draws below stay inside these ranges and needn't reach their ends.
All inputs are finite; a program needn't handle non-finite values.
Results may differ from the reference program's by a relative error of at most 0.0003.
Values sent between devices are 32-bit elements; how exact they have to be, the bound alone decides.
A program may use at most 64 MiB of HBM per device.

```python
import jax
import jax.numpy as jnp
from jax import lax

HEADS = 6
HEAD = 32
D = 192
F = 96
TEST = 256
TRAIN = 16384


def draw_test_cells(key, part):
    base = jax.random.normal(key, (TEST, F, D), jnp.float32)
    return jnp.clip(base, -6.0, 6.0)


def block_scale(key, shape, split, least, largest):
    def one(axis_at, blocks):
        heights = jax.random.uniform(jax.random.fold_in(jax.random.fold_in(key, 6), axis_at), (blocks,), jnp.float32, least / len(split), largest / len(split))
        return jnp.repeat(jnp.exp(heights), shape[axis_at] // blocks).reshape((-1,) + (1,) * (len(shape) - axis_at - 1))

    loudness = one(*split[0])
    for cut in split[1:]:
        loudness = loudness * one(*cut)
    return loudness


def bell_draw(rng, extent, deviation, limit, pieces=(), kind=jnp.bfloat16):
    drawn = jax.random.normal(rng, extent, jnp.float32) * deviation
    if len(pieces) > 0:
        drawn = block_scale(rng, extent, pieces, -0.22, 0.18) * drawn
    return jnp.clip(drawn, min=-limit, max=limit).astype(kind)


def setup_inputs(seed: int = 0) -> dict:
    streams_of = jax.random.split(jax.random.key(seed), 7)
    test_cells = draw_test_cells(jax.random.fold_in(streams_of[6], 71), 0)
    train_cells = bell_draw(streams_of[1], (TRAIN, F, D), 1.0, 6.0, ((0, 32), (1, 8)), jnp.float32)
    w_query = bell_draw(streams_of[2], (D, D), 0.25, 1.5, ((0, 8),), jnp.float32)
    w_key = bell_draw(streams_of[3], (D, D), 0.25, 1.5, ((0, 8),), jnp.float32)
    w_value = bell_draw(streams_of[4], (D, D), D ** -0.5, 0.4375, ((0, 8),), jnp.float32)
    w_out = bell_draw(streams_of[5], (D, D), D ** -0.5, 0.4375, ((0, 8),), jnp.float32)
    return dict(test_cells=test_cells, train_cells=train_cells, w_query=w_query, w_key=w_key, w_value=w_value, w_out=w_out)


def reference(test_cells, train_cells, w_query, w_key, w_value, w_out):
    highest = lax.Precision.HIGHEST
    queries = jnp.einsum('rfd,de->rfe', test_cells, w_query, precision=highest) * (HEAD ** -0.5)
    key_rows = jnp.einsum('rfd,de->rfe', train_cells, w_key, precision=highest)
    value_rows = jnp.einsum('rfd,de->rfe', train_cells, w_value, precision=highest)
    test_rows = queries.shape[0]
    train_rows = key_rows.shape[0]

    def one_feature(feature):
        query_part = lax.dynamic_index_in_dim(queries, feature, 1, keepdims=False).reshape(test_rows, HEADS, HEAD)
        key_part = lax.dynamic_index_in_dim(key_rows, feature, 1, keepdims=False).reshape(train_rows, HEADS, HEAD)
        value_part = lax.dynamic_index_in_dim(value_rows, feature, 1, keepdims=False).reshape(train_rows, HEADS, HEAD)
        scores = jnp.einsum('qhe,khe->hqk', query_part, key_part, precision=highest)
        maxima = jnp.max(scores, axis=-1, keepdims=True)
        probs = jnp.exp(scores - maxima)
        totals = jnp.sum(probs, axis=-1)
        weighted = jnp.einsum('hqk,khe->qhe', probs, value_part, precision=highest)
        mixed = weighted / jnp.transpose(totals)[:, :, None]
        return mixed.reshape(test_rows, HEADS * HEAD)

    mixed = lax.map(one_feature, jnp.arange(F, dtype=jnp.int32))
    return jnp.einsum('ftd,de->tfe', mixed, w_out, precision=highest)
```

```python
import functools

import jax
import jax.numpy as jnp
from jax import lax
from jax.experimental import pallas as pl
from jax.experimental.pallas import tpu as pltpu
from jax.sharding import PartitionSpec as P

BF = jnp.bfloat16
F32 = jnp.float32
HEADS = 6
HEAD = 32
LOG2E = 1.4426950408889634
NZ, NX, NF = 8, 4, 8
VROWS = 2 * HEAD + 16
GROUP = 3
WIDE = 640
MESH = pl.DeviceIdType.MESH


def split(x):
    hi = x.astype(BF)
    return hi, (x - hi.astype(F32)).astype(BF)


def tree(n1, n2):
    low1, high1 = -(n1 // 2), n1 // 2 - 1
    events = []
    for i in range(low1, high1 + 1):
        reach_right, reach_left = (n2 // 2, n2 // 2 - 1) if i % 2 == 0 else (n2 // 2 - 1, n2 // 2)
        for j in range(-reach_right, reach_left + 1):
            children = []
            if j == 0:
                if i <= 0 and i > low1:
                    children.append((0, 1, i - 1, 0))
                if i >= 0 and i < high1:
                    children.append((0, -1, i + 1, 0))
            if j <= 0 and j > -reach_right:
                children.append((1, 1, i, j - 1))
            if j >= 0 and j < reach_left:
                children.append((1, -1, i, j + 1))
            events.append((abs(i) + abs(j), i, j, children))
    return sorted(events)


def kernel(
    x_hbm, t_ref, wq_ref, wk_ref, wv_ref, wo_ref, out_ref,
    xb, wb, gat, kp, vp, qp, wkv, wqc, woc, ot, own, zr, zl, xr, xl,
    x_sem, w_send, w_recv, g_send, g_recv, r_send, r_recv,
):
    width = HEADS * HEAD
    features = x_hbm.shape[0]
    rows = x_hbm.shape[2]
    tests = gat.shape[1] * gat.shape[2]
    feat, place = lax.axis_index("feat"), lax.axis_index("rows")
    z, x = place // NX, place % NX

    def at(dz, dx):
        return lax.rem(z + dz + NZ, NZ) * NX + lax.rem(x + dx + NX, NX)

    for f in range(features):
        pltpu.make_async_copy(x_hbm.at[f], xb.at[f], x_sem.at[f]).start()

    wb[feat] = jnp.concatenate([wk_ref[...], wv_ref[...], wq_ref[...], wo_ref[...]], axis=1)
    for p in range(features // 2):
        gat[p, place] = jnp.concatenate([t_ref[2 * p], t_ref[2 * p + 1]], axis=1)

    barrier = pltpu.get_barrier_semaphore()
    for dz, dx in ((1, 0), (-1, 0), (0, 1), (0, -1)):
        pl.semaphore_signal(
            barrier, inc=1, device_id={"feat": feat, "rows": at(dz, dx)}, device_id_type=MESH
        )
    for k in range(1, NF):
        pl.semaphore_signal(
            barrier,
            inc=1,
            device_id={"feat": lax.rem(feat + k, NF), "rows": place},
            device_id_type=MESH,
        )
    pl.semaphore_wait(barrier, 4 + NF - 1)

    def weight_copy(half, k, source):
        return pltpu.make_async_remote_copy(
            src_ref=wb.at[source, :, pl.ds(half * 2 * width, 2 * width)],
            dst_ref=wb.at[source, :, pl.ds(half * 2 * width, 2 * width)],
            send_sem=w_send.at[half, k - 1],
            recv_sem=w_recv.at[half, k - 1],
            device_id={"feat": lax.rem(feat + k, NF), "rows": place},
            device_id_type=MESH,
        )

    def weights_start(half):
        for k in range(1, NF):
            weight_copy(half, k, feat).start()

    def weights_wait(half):
        for k in range(1, NF):
            weight_copy(half, k, lax.rem(feat - k + NF, NF)).wait_recv()

    half_pairs = features // 4
    plans = (tree(NX, NZ), tree(NZ, NX))
    sends = []

    def block(kind, i, j):
        dz, dx = (j, i) if kind == 0 else (i, j)
        return gat.at[pl.ds(kind * half_pairs, half_pairs), at(dz, dx)]

    def number(kind, i, j):
        dz, dx = (j, i) if kind == 0 else (i, j)
        return (dz % NZ) * NX + dx % NX

    def block_copy(kind, i, j, child):
        axis, step, ci, cj = child
        along_x = (axis == 0) == (kind == 0)
        n = number(kind, ci, cj)
        return pltpu.make_async_remote_copy(
            src_ref=block(kind, i, j),
            dst_ref=block(kind, i, j),
            send_sem=g_send.at[kind, n],
            recv_sem=g_recv.at[kind, n],
            device_id={"feat": feat, "rows": at(0, step) if along_x else at(step, 0)},
            device_id_type=MESH,
        )

    def gather_depth(depth):
        events = [[e for e in plan if e[0] == depth] for plan in plans]
        merged = []
        for n in range(max(len(e) for e in events)):
            for kind in (0, 1):
                if n < len(events[kind]):
                    merged.append((kind, events[kind][n]))
        for kind, (_, i, j, children) in merged:
            if depth > 0:
                n = number(kind, i, j)
                pltpu.make_async_remote_copy(
                    src_ref=block(kind, i, j),
                    dst_ref=block(kind, i, j),
                    send_sem=g_send.at[kind, n],
                    recv_sem=g_recv.at[kind, n],
                    device_id={"feat": feat, "rows": at(1, 0)},
                    device_id_type=MESH,
                ).wait_recv()
            for child in children:
                copy = block_copy(kind, i, j, child)
                copy.start()
                sends.append(copy)

    gather_depth(0)
    weights_start(0)
    weights_start(1)
    gather_depth(1)
    weights_wait(0)
    wt = wb[:, :, : 2 * width].reshape(width, 2 * width).T
    hi, lo = split(wt)
    wkv[...] = jnp.concatenate([hi, lo, hi, lo], axis=1)
    gather_depth(2)

    def keys_values(f, c):
        pltpu.make_async_copy(x_hbm.at[f], xb.at[f], x_sem.at[f]).wait()
        xh, xl_ = split(xb[f])
        kv = jnp.dot(
            wkv[...],
            jnp.concatenate([xh, xh, xl_, xl_], axis=0),
            preferred_element_type=F32,
        )
        kh, kl = split(kv[:width])
        vh, vl = split(kv[width:])
        for h in range(HEADS):
            s = slice(h * HEAD, (h + 1) * HEAD)
            kp[f, h] = jnp.concatenate([kh[s], kh[s], kl[s], kl[s]], axis=0).T
            vp[f, h] = jnp.concatenate([vh[s], vl[s], jnp.ones((16, rows), BF)], axis=0)
        return c

    quarter = features // 4
    for q in range(4):
        lax.fori_loop(q * quarter, (q + 1) * quarter, keys_values, 0)
        gather_depth(3 + q)

    weights_wait(1)
    wt = wb[:, :, 2 * width :].reshape(width, 2 * width)
    hi, lo = split(wt[:, :width].T)
    wqc[...] = jnp.concatenate([hi, lo, hi, lo], axis=1)
    hi, lo = split(wt[:, width:])
    woc[0] = hi
    woc[1] = lo

    def project_queries(p, c):
        both = gat[p].reshape(tests, 2 * width).T
        for u in range(2):
            th, tl = split(both[u * width : (u + 1) * width])
            q = jnp.dot(
                wqc[...], jnp.concatenate([th, th, tl, tl], axis=0), preferred_element_type=F32
            ) * (HEAD**-0.5 * LOG2E)
            qh, ql = split(q)
            for h in range(HEADS):
                s = slice(h * HEAD, (h + 1) * HEAD)
                qp[2 * p + u, h] = jnp.concatenate([qh[s], ql[s], qh[s], ql[s]], axis=0)
        return c

    lax.fori_loop(0, features // 2, project_queries, 0)

    def attend(f, c):
        u = lax.rem(f, GROUP)
        for h in range(HEADS):
            s = jnp.dot(kp[f, h], qp[f, h], preferred_element_type=F32)
            m = jnp.max(s, axis=0, keepdims=True)
            ph, pl_ = split(jnp.exp2(s - m))
            vv = vp[f, h]
            o = jnp.dot(vv, ph, preferred_element_type=F32) + jnp.dot(
                vv, pl_, preferred_element_type=F32
            )
            row = pl.multiple_of(u * width, 8) + h * HEAD
            ot[pl.ds(row, HEAD), :] = o[:HEAD] + o[HEAD : 2 * HEAD]
            ot[pl.ds(GROUP * width + u * HEADS + h, 1), :] = m
            ot[pl.ds(GROUP * width + (GROUP + u) * HEADS + h, 1), :] = o[2 * HEAD : 2 * HEAD + 1]
        return c

    stat0 = GROUP * width - (WIDE - 128)
    stats = GROUP * HEADS

    def spread_index(tile, n):
        lane = lax.broadcasted_iota(jnp.int32, (n, 128), 1)
        if tile < WIDE // 128 - 1:
            return stat0 + (lane + tile * 128) // HEAD
        low = stat0 + (lane + tile * 128) // HEAD
        high = stat0 + lane - (stat0 + stats)
        return jnp.where(lane < stat0, low, jnp.clip(high, 0, 127))

    def spread(factor, tile):
        idx = spread_index(tile, factor.shape[0])
        return jnp.take_along_axis(factor, idx, axis=1, mode="promise_in_bounds")

    def merge(dst, srcs, n):
        tail = pl.ds(WIDE - 128, 128)
        mine = dst[:, :, tail].reshape(n * 8, 128)
        theirs = [s[:, :, tail].reshape(n * 8, 128) for s in srcs]
        top = functools.reduce(jnp.maximum, theirs, mine)
        factors = [jnp.exp2(v - top) for v in (mine, *theirs)]
        lane = lax.broadcasted_iota(jnp.int32, (n * 8, 128), 1)
        is_max = (lane >= stat0) & (lane < stat0 + stats)
        for tile in range(WIDE // 128):
            at_ = pl.ds(tile * 128, 128)
            total = None
            for ref, factor in zip((dst, *srcs), factors):
                term = ref[:, :, at_].reshape(n * 8, 128) * spread(factor, tile)
                total = term if total is None else total + term
            if tile == WIDE // 128 - 1:
                total = jnp.where(is_max, top, total)
            dst[:, :, at_] = total.reshape(n, 8, 128)

    def column(g, dz):
        return own.at[g, pl.ds(lax.rem(z + dz + NZ, NZ) * NX, NX)]

    def cell(g, dx):
        return own.at[g, pl.ds(at(0, dx), 1)]

    def reduce_copy(g, n, src, dst, dz, dx):
        return pltpu.make_async_remote_copy(
            src_ref=src,
            dst_ref=dst,
            send_sem=r_send.at[g, n],
            recv_sem=r_recv.at[g, n],
            device_id={"feat": feat, "rows": at(dz, dx)},
            device_id_type=MESH,
        )

    def z_right(g, s):
        return reduce_copy(g, s, column(g, 4 - s), zr.at[g, s], 1, 0)

    def z_left(g, s):
        return reduce_copy(g, 4 + s, column(g, s - 3), zl.at[g, s], -1, 0)

    def x_right(g, s):
        return reduce_copy(g, 7 + s, cell(g, 2 - s), xr.at[g, s], 0, 1)

    def x_left(g):
        return reduce_copy(g, 9, cell(g, -1), xl.at[g], 0, -1)

    def start(copy):
        copy.start()
        sends.append(copy)

    def tick(g, s):
        if s == 0:
            own[g] = ot[...].T.reshape(own.shape[1:])
            start(z_right(g, 0))
            start(z_left(g, 0))
        elif s <= 3:
            z_right(g, s - 1).wait_recv()
            merge(column(g, 4 - s), [zr.at[g, s - 1]], NX)
            start(z_right(g, s))
            if s <= 2:
                z_left(g, s - 1).wait_recv()
                merge(column(g, s - 3), [zl.at[g, s - 1]], NX)
                start(z_left(g, s))
        elif s == 4:
            z_left(g, 2).wait_recv()
            z_right(g, 3).wait_recv()
            merge(column(g, 0), [zr.at[g, 3], zl.at[g, 2]], NX)
            start(x_right(g, 0))
            start(x_left(g))
        elif s == 5:
            x_right(g, 0).wait_recv()
            merge(cell(g, 1), [xr.at[g, 0]], 1)
            start(x_right(g, 1))
        elif s == 6:
            x_left(g).wait_recv()
            x_right(g, 1).wait_recv()
            merge(cell(g, 0), [xr.at[g, 1], xl.at[g]], 1)

    groups = features // GROUP
    progress = [0] * groups

    def tick_all(upto):
        for g in range(upto):
            if progress[g] <= 6:
                tick(g, progress[g])
                progress[g] += 1

    for g in range(groups):
        if g == 0:
            lax.fori_loop(0, GROUP, attend, 0)
        else:
            lax.fori_loop(g * GROUP, g * GROUP + 2, attend, 0)
            tick_all(g)
            lax.fori_loop(g * GROUP + 2, (g + 1) * GROUP, attend, 0)
        tick_all(g + 1)
    while min(progress) <= 6:
        tick_all(groups)

    wh, wl = woc[0], woc[1]
    for g in range(groups):
        mine = own.at[g, place]
        inverse = 1.0 / mine[:, WIDE - 128 :]
        parts = []
        for tile in range(WIDE // 128):
            index = spread_index(tile, 8) + stats
            if tile == WIDE // 128 - 1:
                index = jnp.clip(index, 0, 127)
            scale = jnp.take_along_axis(inverse, index, axis=1, mode="promise_in_bounds")
            parts.append(mine[:, tile * 128 : (tile + 1) * 128] * scale)
        mixed = jnp.concatenate(parts, axis=1)
        for u in range(GROUP):
            mh, ml = split(mixed[:, u * width : (u + 1) * width])
            out_ref[g * GROUP + u] = (
                jnp.dot(mh, wh, preferred_element_type=F32)
                + jnp.dot(mh, wl, preferred_element_type=F32)
                + jnp.dot(ml, wh, preferred_element_type=F32)
                + jnp.dot(ml, wl, preferred_element_type=F32)
            )
    for half in range(2):
        for k in range(1, NF):
            weight_copy(half, k, feat).wait_send()
    for copy in sends:
        copy.wait_send()


def per_device(test_cells, train_cells, w_query, w_key, w_value, w_out):
    cells = jnp.transpose(train_cells, (1, 2, 0))
    tests = jnp.transpose(test_cells, (1, 0, 2))
    features, width, rows = cells.shape
    mine = tests.shape[1]
    owners = NZ * NX
    all_tests = owners * mine
    groups = features // GROUP
    vmem = pl.BlockSpec(memory_space=pltpu.VMEM)
    dma = pltpu.SemaphoreType.DMA
    out = pl.pallas_call(
        kernel,
        out_shape=jax.ShapeDtypeStruct((features, mine, width), F32),
        in_specs=[pl.BlockSpec(memory_space=pl.ANY)] + [vmem] * 5,
        out_specs=vmem,
        scratch_shapes=[
            pltpu.VMEM((features, width, rows), F32),
            pltpu.VMEM((NF, width // NF, 4 * width), F32),
            pltpu.VMEM((features // 2, owners, mine, 2 * width), F32),
            pltpu.VMEM((features, HEADS, rows, 4 * HEAD), BF),
            pltpu.VMEM((features, HEADS, VROWS, rows), BF),
            pltpu.VMEM((features, HEADS, 4 * HEAD, all_tests), BF),
            pltpu.VMEM((2 * width, 4 * width), BF),
            pltpu.VMEM((width, 4 * width), BF),
            pltpu.VMEM((2, width, width), BF),
            pltpu.VMEM((WIDE, all_tests), F32),
            pltpu.VMEM((groups, owners, mine, WIDE), F32),
            pltpu.VMEM((groups, 4, NX, mine, WIDE), F32),
            pltpu.VMEM((groups, 3, NX, mine, WIDE), F32),
            pltpu.VMEM((groups, 2, 1, mine, WIDE), F32),
            pltpu.VMEM((groups, 1, mine, WIDE), F32),
            dma((features,)),
            dma((2, NF - 1)),
            dma((2, NF - 1)),
            dma((2, owners)),
            dma((2, owners)),
            dma((groups, 10)),
            dma((groups, 10)),
        ],
        compiler_params=pltpu.CompilerParams(
            collective_id=0, has_side_effects=True, vmem_limit_bytes=60 * 2**20
        ),
        name="attention",
    )(cells, tests, w_query, w_key, w_value, w_out)
    return jnp.transpose(out, (1, 0, 2))


def solution(mesh):
    rows = P("rows", "feat", None)
    weights = P("feat", None)
    return jax.shard_map(
        per_device,
        mesh=mesh,
        in_specs=(rows, rows, weights, weights, weights, weights),
        out_specs=rows,
        check_vma=False,
    )
```

```python
import functools

import jax
import jax.numpy as jnp
from jax import lax
from jax.experimental import pallas as pl
from jax.experimental.pallas import tpu as pltpu
from jax.sharding import PartitionSpec as P

BF = jnp.bfloat16
F32 = jnp.float32
HEADS = 6
HEAD = 32
LOG2E = 1.4426950408889634
NZ, NX, NF = 8, 4, 8
VROWS = 2 * HEAD + 16
GROUPS = (3, 3, 2, 2, 1, 1)
Z_FIRST = 2
MESH = pl.DeviceIdType.MESH


def split(x):
    hi = x.astype(BF)
    return hi, (x - hi.astype(F32)).astype(BF)


def lanes(count):
    return -(-count * HEADS * (HEAD + 2) // 128) * 128


def kernel(
    x_hbm, t_ref, wq_ref, wk_ref, wv_ref, wo_ref, out_ref,
    xb, wb, gat, kp, vp, qp, wkv, wqc, woc, ot,
    x_sem, w_send, w_recv, g_send, g_recv, r_send, r_recv, own, inbox,
):
    width = HEADS * HEAD
    features = x_hbm.shape[0]
    rows = x_hbm.shape[2]
    tests = gat.shape[1] * gat.shape[2] * gat.shape[3]
    feat, place = lax.axis_index("feat"), lax.axis_index("rows")
    z, x = place // NX, place % NX
    nothing = place // (NZ * NX)

    def at(dz, dx):
        return lax.rem(z + dz + NZ, NZ) * NX + lax.rem(x + dx + NX, NX)

    for f in range(features):
        pltpu.make_async_copy(x_hbm.at[f], xb.at[f], x_sem.at[f]).start()

    wb[0, feat] = jnp.concatenate([wk_ref[...], wv_ref[...]], axis=1)
    wb[1, feat] = jnp.concatenate([wq_ref[...], wo_ref[...]], axis=1)
    pairs = features // 2
    for p in range(pairs):
        gat[p, z, x] = jnp.concatenate([t_ref[2 * p], t_ref[2 * p + 1]], axis=1)

    def there(dz, dx):
        return {"feat": feat, "rows": at(dz, dx)}

    def peer(k):
        return {"feat": lax.rem(feat + k, NF), "rows": place}

    with jax.named_scope("bar"):
        barrier = pltpu.get_barrier_semaphore()
        peers = [there(dz, 0) for dz in range(1, NZ)] + [there(0, 1), there(0, -1)]
        peers += [peer(k) for k in range(1, NF)]
        for other in peers:
            pl.semaphore_signal(barrier, inc=1, device_id=other, device_id_type=MESH)
        pl.semaphore_wait(barrier, len(peers))

    def remote(src, dst, send_sem, recv_sem, device):
        return pltpu.make_async_remote_copy(
            src_ref=src,
            dst_ref=dst,
            send_sem=send_sem,
            recv_sem=recv_sem,
            device_id=device,
            device_id_type=MESH,
        )

    def weights_start(half):
        for k in range(1, NF):
            mine = wb.at[half, feat]
            remote(mine, mine, w_send.at[half], w_recv.at[half], peer(k)).start()

    def weights_all(half):
        seven = wb.at[half, pl.ds(0, NF - 1)]
        return remote(seven, seven, w_send.at[half], w_recv.at[half], peer(1))

    def stage(p, n, ref, device):
        return remote(ref, ref, g_send.at[p, n], g_recv.at[p, n], device)

    def stage_all(p, n):
        ref = (gat.at[p, pl.ds(0, NZ - 1), 0], gat.at[p, pl.ds(0, 4)], gat.at[p, pl.ds(0, 2)])[n]
        return stage(p, n, ref, there(1, 0))

    def column_of(dx):
        return lax.rem(x + dx + NX, NX)

    def along_z(p):
        for dz in range(1, NZ):
            stage(p, 0, gat.at[p, z, x], there(dz, 0)).start()

    def along_x(p):
        with jax.named_scope("x1_%d" % p):
            stage_all(p, 0).wait_recv()
        for dx in (1, -1):
            stage(p, 1, gat.at[p, :, x], there(0, dx)).start()

    def further_x(p):
        with jax.named_scope("x2_%d" % p):
            stage_all(p, 1).wait_recv()
        half = NZ // 2
        stage(p, 2, gat.at[p, pl.ds(0, half), column_of(-1)], there(0, 1)).start()
        stage(p, 2, gat.at[p, pl.ds(half, half), column_of(1)], there(0, -1)).start()

    def arrived(p):
        with jax.named_scope("x3_%d" % p):
            stage_all(p, 2).wait_recv()

    weights_start(0)
    for p in range(pairs):
        along_z(p)
    along_x(0)
    with jax.named_scope("w0"):
        weights_all(0).wait_recv()
    weights_start(1)
    hi, lo = split(wb[0].reshape(width, 2 * width).T)
    wkv[...] = jnp.concatenate([hi, lo, hi, lo], axis=1)

    def keys_values(f, c):
        pltpu.make_async_copy(x_hbm.at[f], xb.at[f], x_sem.at[f]).wait()
        xh, xl_ = split(xb[f])
        kv = jnp.dot(
            wkv[...],
            jnp.concatenate([xh, xh, xl_, xl_], axis=0),
            preferred_element_type=F32,
        )
        kh, kl = split(kv[:width])
        vh, vl = split(kv[width:])
        for h in range(HEADS):
            s = slice(h * HEAD, (h + 1) * HEAD)
            kp[f, h] = jnp.concatenate([kh[s], kh[s], kl[s], kl[s]], axis=0).T
            vp[f, h] = jnp.concatenate([vh[s], vl[s], jnp.ones((16, rows), BF)], axis=0)
        return c

    moves = [
        [(along_x, 1)],
        [(further_x, 0), (along_x, 2)],
        [(along_x, 3)],
        [(further_x, 1)],
        [(along_x, 4)],
        [(further_x, 2), (along_x, 5)],
    ]
    for p in range(pairs):
        with jax.named_scope("kv"):
            lax.fori_loop(2 * p, 2 * p + 2, keys_values, 0)
        for move, n in moves[p]:
            move(n)

    with jax.named_scope("w1"):
        weights_all(1).wait_recv()
    wt = wb[1].reshape(width, 2 * width)
    hi, lo = split(wt[:, :width].T)
    wqc[...] = jnp.concatenate([hi, lo, hi, lo], axis=1)
    hi, lo = split(wt[:, width:])
    woc[0] = hi
    woc[1] = lo

    def project_queries(p):
        arrived(p)
        both = gat[p].reshape(tests, 2 * width).T
        for u in range(2):
            th, tl = split(both[u * width : (u + 1) * width])
            q = jnp.dot(
                wqc[...], jnp.concatenate([th, th, tl, tl], axis=0), preferred_element_type=F32
            ) * (HEAD**-0.5 * LOG2E)
            qh, ql = split(q)
            for h in range(HEADS):
                s = slice(h * HEAD, (h + 1) * HEAD)
                qp[2 * p + u, h] = jnp.concatenate([qh[s], ql[s], qh[s], ql[s]], axis=0)

    def attend(first, count, f):
        u = f - first
        for h in range(HEADS):
            s = jnp.dot(kp[f, h], qp[f, h], preferred_element_type=F32)
            m = jnp.max(s, axis=0, keepdims=True)
            ph, pl_ = split(jnp.exp2(s - m))
            vv = vp[f, h]
            o = jnp.dot(vv, ph, preferred_element_type=F32) + jnp.dot(
                vv, pl_, preferred_element_type=F32
            )
            row = pl.multiple_of(u * width, 8) + h * HEAD
            ot[pl.ds(row, HEAD), :] = o[:HEAD] + o[HEAD : 2 * HEAD]
            ot[pl.ds(count * width + u * HEADS + h, 1), :] = m
            ot[pl.ds(count * width + (count + u) * HEADS + h, 1), :] = o[2 * HEAD : 2 * HEAD + 1]

    def spread_index(count, tile, n):
        lane = lax.broadcasted_iota(jnp.int32, (n, 128), 1)
        wide = lanes(count)
        first = count * width - (wide - 128)
        low = first + (lane + tile * 128) // HEAD
        if tile < wide // 128 - 1:
            return low
        high = lane - count * HEADS
        return jnp.clip(jnp.where(lane < first, low, high), 0, 127)

    def merge(count, dst, srcs):
        wide = lanes(count)
        first = count * width - (wide - 128)
        shape = dst.shape[:-1]
        n = dst.size // wide
        tail = pl.ds(wide - 128, 128)

        def load(ref, part):
            return ref[..., part].reshape(n, 128)

        refs = (dst, *srcs)
        stats = [load(r, tail) for r in refs]
        top = functools.reduce(jnp.maximum, stats)
        factors = [jnp.exp2(v - top) for v in stats]
        lane = lax.broadcasted_iota(jnp.int32, (n, 128), 1)
        is_max = (lane >= first) & (lane < first + count * HEADS)
        for tile in range(wide // 128):
            part = pl.ds(tile * 128, 128)
            index = spread_index(count, tile, n)
            total = None
            for ref, factor in zip(refs, factors):
                scale = jnp.take_along_axis(factor, index, axis=1, mode="promise_in_bounds")
                term = load(ref, part) * scale
                total = term if total is None else total + term
            if tile == wide // 128 - 1:
                total = jnp.where(is_max, top, total)
            dst[..., part] = total.reshape(*shape, 128)

    def z_of(dz):
        return lax.rem(z + dz + NZ, NZ)

    def x_of(dx):
        return lax.rem(x + dx + NX, NX)

    def send(g, n, src, dst, dz, dx):
        remote(src, dst, r_send.at[g], r_recv.at[g, n], there(dz, dx)).start()

    def receive(g, n, dst):
        remote(dst, dst, r_send.at[g], r_recv.at[g, n], there(1, 0)).wait_recv()

    def z_first(g, s):
        count, mine = GROUPS[g], own[g]
        zr, zl, xr, xl = inbox[g]
        if s <= 3:
            if s > 0:
                receive(g, s - 1, zr.at[s - 1])
                merge(count, mine.at[z_of(4 - s)], [zr.at[s - 1]])
            send(g, s, mine.at[z_of(4 - s)], zr.at[s], 1, 0)
            if s < 3:
                if s > 0:
                    receive(g, 3 + s, zl.at[s - 1])
                    merge(count, mine.at[z_of(s - 3)], [zl.at[s - 1]])
                send(g, 4 + s, mine.at[z_of(s - 3)], zl.at[s], -1, 0)
        elif s == 4:
            receive(g, 6, zl.at[2])
            receive(g, 3, zr.at[3])
            merge(count, mine.at[z], [zr.at[3], zl.at[2]])
            send(g, 7, mine.at[z, x_of(2)], xr.at[0], 0, 1)
            send(g, 9, mine.at[z, x_of(-1)], xl, 0, -1)
        elif s == 5:
            receive(g, 7, xr.at[0])
            merge(count, mine.at[z, x_of(1)], [xr.at[0]])
            send(g, 8, mine.at[z, x_of(1)], xr.at[1], 0, 1)
        else:
            receive(g, 9, xl)
            receive(g, 8, xr.at[1])
            merge(count, mine.at[z, x], [xr.at[1], xl])

    def x_first(g, s):
        count, mine = GROUPS[g], own[g]
        half, right, left, rest = inbox[g]
        low, high = pl.ds(0, NZ // 2), pl.ds(NZ // 2, NZ // 2)
        if s == 0:
            send(g, 0, mine.at[low, x_of(2)], half.at[0], 0, 1)
            send(g, 1, mine.at[high, x_of(2)], half.at[1], 0, -1)
        elif s == 1:
            receive(g, 0, half.at[0])
            merge(count, mine.at[low, x_of(1)], [half.at[0]])
            send(g, 2, mine.at[:, x_of(1)], right, 0, 1)
            receive(g, 1, half.at[1])
            merge(count, mine.at[high, x_of(-1)], [half.at[1]])
            send(g, 3, mine.at[:, x_of(-1)], left, 0, -1)
        elif s == 2:
            receive(g, 2, right)
            receive(g, 3, left)
            merge(count, mine.at[:, x], [right, left])
            for dz in (4, 3, 5, 2, 6, 1, 7):
                send(g, 4, mine.at[z_of(dz), x], rest.at[dz - 1], dz, 0)
        else:
            receive(g, 4, rest)
            merge(count, mine.at[z, x], [rest.at[k] for k in range(NZ - 1)])

    starts = [sum(GROUPS[:g]) for g in range(len(GROUPS))]

    def finish(g):
        count = GROUPS[g]
        wide = lanes(count)
        mine = own[g].at[z, x]
        inverse = 1.0 / mine[:, wide - 128 :]
        parts = []
        for tile in range(wide // 128):
            index = jnp.clip(spread_index(count, tile, 8) + count * HEADS, 0, 127)
            scale = jnp.take_along_axis(inverse, index, axis=1, mode="promise_in_bounds")
            parts.append(mine[:, tile * 128 : (tile + 1) * 128] * scale)
        mixed = jnp.concatenate(parts, axis=1)
        for u in range(count):
            mh, ml = split(mixed[:, u * width : (u + 1) * width])
            out_ref[starts[g] + u] = (
                jnp.dot(mh, woc[0], preferred_element_type=F32)
                + jnp.dot(mh, woc[1], preferred_element_type=F32)
                + jnp.dot(ml, woc[0], preferred_element_type=F32)
                + jnp.dot(ml, woc[1], preferred_element_type=F32)
            )

    def tick(g, s):
        with jax.named_scope("t%d_%d" % (g, s)):
            if s == 0:
                own[g][...] = ot[: lanes(GROUPS[g]), :].T.reshape(own[g].shape)
            (z_first if g < Z_FIRST else x_first)(g, s)
            if s == (6 if g < Z_FIRST else 3):
                finish(g)

    def att(first, last):
        group = max(g for g in range(len(GROUPS)) if starts[g] <= first)

        def body(f, c):
            attend(starts[group], GROUPS[group], f)
            return c

        with jax.named_scope("att"):
            lax.fori_loop(first, last + nothing, body, 0)

    schedule = [
        (0, 2, []),
        (2, 3, [(0, 0)]),
        (3, 4, []),
        (4, 6, [(1, 0), (0, 1)]),
        (6, 8, [(2, 0), (0, 2), (1, 1)]),
        (8, 10, [(3, 0), (0, 3), (1, 2), (2, 1)]),
        (10, 11, [(4, 0), (0, 4), (3, 1)]),
        (11, 12, [(5, 0), (2, 2), (1, 3), (0, 5), (4, 1), (3, 2), (5, 1), (1, 4), (0, 6), (2, 3)]
         + [(4, 2), (5, 2), (1, 5), (3, 3), (4, 3), (1, 6), (5, 3)]),
    ]
    for first, last, ticks in schedule:
        if first % 2 == 0:
            p = first // 2
            if 0 < p < 4:
                further_x(p + 2)
            with jax.named_scope("pq"):
                project_queries(p)
        att(first, last)
        for g, s in ticks:
            tick(g, s)

    for half in range(2):
        weights_all(half).wait_send()
    for p in range(pairs):
        for n in range(3):
            stage_all(p, n).wait_send()
    for g in range(len(GROUPS)):
        sent = [own[g].at[pl.ds(0, 7)], own[g].at[0, pl.ds(0, 3)]]
        if g >= Z_FIRST:
            sent = [own[g].at[pl.ds(0, 6)], own[g].at[pl.ds(0, 7), 0]]
        for ref in sent:
            remote(ref, ref, r_send.at[g], r_recv.at[g, 0], there(1, 0)).wait_send()


def per_device(test_cells, train_cells, w_query, w_key, w_value, w_out):
    cells = jnp.transpose(train_cells, (1, 2, 0))
    tests = jnp.transpose(test_cells, (1, 0, 2))
    features, width, rows = cells.shape
    mine = tests.shape[1]
    owners = NZ * NX
    all_tests = owners * mine
    inboxes = []
    for g, count in enumerate(GROUPS):
        outer = [(4, NX), (3, NX), (2,), ()] if g < Z_FIRST else [(2, 4), (NZ,), (NZ,), (NZ - 1,)]
        inboxes.append([pltpu.VMEM((*o, mine, lanes(count)), F32) for o in outer])
    vmem = pl.BlockSpec(memory_space=pltpu.VMEM)
    dma = pltpu.SemaphoreType.DMA
    out = pl.pallas_call(
        kernel,
        out_shape=jax.ShapeDtypeStruct((features, mine, width), F32),
        in_specs=[pl.BlockSpec(memory_space=pl.ANY)] + [vmem] * 5,
        out_specs=vmem,
        scratch_shapes=[
            pltpu.VMEM((features, width, rows), F32),
            pltpu.VMEM((2, NF, width // NF, 2 * width), F32),
            pltpu.VMEM((features // 2, NZ, NX, mine, 2 * width), F32),
            pltpu.VMEM((features, HEADS, rows, 4 * HEAD), BF),
            pltpu.VMEM((features, HEADS, VROWS, rows), BF),
            pltpu.VMEM((features, HEADS, 4 * HEAD, all_tests), BF),
            pltpu.VMEM((2 * width, 4 * width), BF),
            pltpu.VMEM((width, 4 * width), BF),
            pltpu.VMEM((2, width, width), BF),
            pltpu.VMEM((lanes(max(GROUPS)), all_tests), F32),
            dma((features,)),
            dma((2,)),
            dma((2,)),
            dma((features // 2, 3)),
            dma((features // 2, 3)),
            dma((len(GROUPS),)),
            dma((len(GROUPS), 10)),
            [pltpu.VMEM((NZ, NX, mine, lanes(n)), F32) for n in GROUPS],
            inboxes,
        ],
        compiler_params=pltpu.CompilerParams(
            collective_id=0, has_side_effects=True, vmem_limit_bytes=60 * 2**20
        ),
        name="attention",
    )(cells, tests, w_query, w_key, w_value, w_out)
    return jnp.transpose(out, (1, 0, 2))


def solution(mesh):
    rows = P("rows", "feat", None)
    weights = P("feat", None)
    return jax.shard_map(
        per_device,
        mesh=mesh,
        in_specs=(rows, rows, weights, weights, weights, weights),
        out_specs=rows,
        check_vma=False,
    )
```

```python
import functools

import jax
import jax.numpy as jnp
from jax import lax
from jax.experimental import pallas as pl
from jax.experimental.pallas import tpu as pltpu
from jax.sharding import PartitionSpec as P

BF = jnp.bfloat16
F32 = jnp.float32
HEADS = 6
HEAD = 32
LOG2E = 1.4426950408889634
NZ, NX, NF = 8, 4, 8
VROWS = 4 * HEAD + 16
GROUPS = (3, 3, 2, 2, 1, 1)
Z_FIRST = (0, 2)
MESH = pl.DeviceIdType.MESH


def split(x):
    hi = x.astype(BF)
    return hi, (x - hi.astype(F32)).astype(BF)


def lanes(count):
    return -(-count * HEADS * (HEAD + 2) // 128) * 128


def kernel(
    x_hbm, t_ref, wq_ref, wk_ref, wv_ref, wo_ref, out_ref,
    xb, wb, gat, kp, vp, qp, wkv, wqc, woc, ot, kv, sc,
    x_sem, w_send, w_recv, g_send, g_recv, r_send, r_recv, own, inbox,
):
    width = HEADS * HEAD
    features = x_hbm.shape[0]
    rows = x_hbm.shape[2]
    tests = gat.shape[1] * gat.shape[2] * gat.shape[3]
    feat, place = lax.axis_index("feat"), lax.axis_index("rows")
    z, x = place // NX, place % NX
    nothing = place // (NZ * NX)

    def at(dz, dx):
        return lax.rem(z + dz + NZ, NZ) * NX + lax.rem(x + dx + NX, NX)

    for f in range(features):
        pltpu.make_async_copy(x_hbm.at[f], xb.at[f], x_sem.at[f]).start()

    wb[0, feat] = jnp.concatenate([wk_ref[...], wv_ref[...]], axis=1)
    wb[1, feat] = jnp.concatenate([wq_ref[...], wo_ref[...]], axis=1)
    pairs = features // 2
    for p in range(pairs):
        gat[p, z, x] = jnp.concatenate([t_ref[2 * p], t_ref[2 * p + 1]], axis=1)

    def there(dz, dx):
        return {"feat": feat, "rows": at(dz, dx)}

    def peer(k):
        return {"feat": lax.rem(feat + k, NF), "rows": place}

    with jax.named_scope("bar"):
        barrier = pltpu.get_barrier_semaphore()
        peers = [there(dz, 0) for dz in range(1, NZ)] + [there(0, 1), there(0, -1)]
        peers += [peer(k) for k in range(1, NF)]
        for other in peers:
            pl.semaphore_signal(barrier, inc=1, device_id=other, device_id_type=MESH)
        pl.semaphore_wait(barrier, len(peers))

    def remote(src, dst, send_sem, recv_sem, device):
        return pltpu.make_async_remote_copy(
            src_ref=src,
            dst_ref=dst,
            send_sem=send_sem,
            recv_sem=recv_sem,
            device_id=device,
            device_id_type=MESH,
        )

    def weights_start(half):
        for k in range(1, NF):
            mine = wb.at[half, feat]
            remote(mine, mine, w_send.at[half], w_recv.at[half], peer(k)).start()

    def weights_all(half):
        seven = wb.at[half, pl.ds(0, NF - 1)]
        return remote(seven, seven, w_send.at[half], w_recv.at[half], peer(1))

    def stage(p, n, ref, device):
        return remote(ref, ref, g_send.at[p, n], g_recv.at[p, n], device)

    def stage_all(p, n):
        ref = (gat.at[p, pl.ds(0, NZ - 1), 0], gat.at[p, pl.ds(0, 4)], gat.at[p, pl.ds(0, 2)])[n]
        return stage(p, n, ref, there(1, 0))

    def column_of(dx):
        return lax.rem(x + dx + NX, NX)

    def along_z(p):
        for dz in range(1, NZ):
            stage(p, 0, gat.at[p, z, x], there(dz, 0)).start()

    def along_x(p):
        with jax.named_scope("x1_%d" % p):
            stage_all(p, 0).wait_recv()
        for dx in (1, -1):
            stage(p, 1, gat.at[p, :, x], there(0, dx)).start()

    def further_x(p):
        with jax.named_scope("x2_%d" % p):
            stage_all(p, 1).wait_recv()
        half = NZ // 2
        stage(p, 2, gat.at[p, pl.ds(0, half), column_of(-1)], there(0, 1)).start()
        stage(p, 2, gat.at[p, pl.ds(half, half), column_of(1)], there(0, -1)).start()

    def arrived(p):
        with jax.named_scope("x3_%d" % p):
            stage_all(p, 2).wait_recv()

    weights_start(0)
    for p in range(pairs):
        along_z(p)
    along_x(0)
    with jax.named_scope("w0"):
        weights_all(0).wait_recv()
    weights_start(1)
    hi, lo = split(wb[0].reshape(width, 2 * width).T)
    wkv[...] = jnp.concatenate([hi, lo, hi, lo], axis=1)

    def project(f, slot):
        xh, xl_ = split(xb[f])
        kv[slot] = jnp.dot(
            wkv[...],
            jnp.concatenate([xh, xh, xl_, xl_], axis=0),
            preferred_element_type=F32,
        )

    def pack(f, slot):
        kh, kl = split(kv[slot, :width])
        vh, vl = split(kv[slot, width:])
        for h in range(HEADS):
            s = slice(h * HEAD, (h + 1) * HEAD)
            kp[f, h] = jnp.concatenate([kh[s], kh[s], kl[s], kl[s]], axis=0).T
        for g in range(HEADS // 2):
            a = slice(2 * g * HEAD, (2 * g + 1) * HEAD)
            b = slice((2 * g + 1) * HEAD, (2 * g + 2) * HEAD)
            vp[f, g] = jnp.concatenate([vh[a], vl[a], vh[b], vl[b], jnp.ones((16, rows), BF)], axis=0)

    def keys_values(p, c):
        f = 2 * p
        project(f + 1, 1)
        pack(f, 0)
        project(jnp.minimum(f + 2, features - 1), 0)
        pack(f + 1, 1)
        return c

    for f in range(features):
        pltpu.make_async_copy(x_hbm.at[f], xb.at[f], x_sem.at[f]).wait()
    project(0, 0)
    moves = [
        [(along_x, 1)],
        [],
        [(further_x, 0), (along_x, 2)],
        [],
        [],
        [(further_x, 1), (along_x, 3)],
    ]
    for p in range(pairs):
        with jax.named_scope("kv"):
            lax.fori_loop(p, p + 1 + nothing, keys_values, 0)
        for move, n in moves[p]:
            move(n)

    with jax.named_scope("w1"):
        weights_all(1).wait_recv()
    wt = wb[1].reshape(width, 2 * width)
    hi, lo = split(wt[:, :width].T)
    wqc[...] = jnp.concatenate([hi, lo, hi, lo], axis=1)
    hi, lo = split(wt[:, width:])
    woc[0] = hi
    woc[1] = lo

    def project_queries(p):
        arrived(p)
        both = gat[p].reshape(tests, 2 * width).T
        for u in range(2):
            th, tl = split(both[u * width : (u + 1) * width])
            q = jnp.dot(
                wqc[...], jnp.concatenate([th, th, tl, tl], axis=0), preferred_element_type=F32
            ) * (HEAD**-0.5 * LOG2E)
            qh, ql = split(q)
            for h in range(HEADS):
                s = slice(h * HEAD, (h + 1) * HEAD)
                qp[2 * p + u, h] = jnp.concatenate([qh[s], ql[s], qh[s], ql[s]], axis=0)

    def scores(f, g):
        for u in range(2):
            h = 2 * g + u
            sc[g, u] = jnp.dot(kp[f, h], qp[f, h], preferred_element_type=F32)

    def attend(first, count, f):
        place_of = pl.multiple_of((f - first) * width, 8)
        stat = count * width + (f - first) * HEADS
        following = jnp.minimum(f + 1, features - 1)
        pairs_of_heads = HEADS // 2
        for g in range(pairs_of_heads):
            if g + 1 < pairs_of_heads:
                scores(f, g + 1)
            else:
                scores(following, 0)
            tops = [jnp.max(sc[g, u], axis=0, keepdims=True) for u in range(2)]
            probs = [split(jnp.exp2(sc[g, u] - tops[u])) for u in range(2)]
            both = [jnp.concatenate([p[part] for p in probs], axis=1) for part in range(2)]
            vv = vp[f, g]
            o = jnp.dot(
                jnp.concatenate([vv, vv], axis=1),
                jnp.concatenate(both, axis=0),
                preferred_element_type=F32,
            )
            for u in range(2):
                part = o[2 * u * HEAD : (2 * u + 2) * HEAD, u * tests : (u + 1) * tests]
                h = 2 * g + u
                ot[pl.ds(place_of + h * HEAD, HEAD), :] = part[:HEAD] + part[HEAD:]
                ot[pl.ds(stat + h, 1), :] = tops[u]
                ot[pl.ds(stat + count * HEADS + h, 1), :] = o[
                    4 * HEAD : 4 * HEAD + 1, u * tests : (u + 1) * tests
                ]

    def spread_index(count, tile, n):
        lane = lax.broadcasted_iota(jnp.int32, (n, 128), 1)
        wide = lanes(count)
        first = count * width - (wide - 128)
        low = first + (lane + tile * 128) // HEAD
        if tile < wide // 128 - 1:
            return low
        high = lane - count * HEADS
        return jnp.clip(jnp.where(lane < first, low, high), 0, 127)

    def merge(count, dst, srcs):
        wide = lanes(count)
        first = count * width - (wide - 128)
        shape = dst.shape[:-1]
        n = dst.size // wide
        tail = pl.ds(wide - 128, 128)

        def load(ref, part):
            return ref[..., part].reshape(n, 128)

        refs = (dst, *srcs)
        stats = [load(r, tail) for r in refs]
        top = functools.reduce(jnp.maximum, stats)
        factors = [jnp.exp2(v - top) for v in stats]
        lane = lax.broadcasted_iota(jnp.int32, (n, 128), 1)
        is_max = (lane >= first) & (lane < first + count * HEADS)
        for tile in range(wide // 128):
            part = pl.ds(tile * 128, 128)
            index = spread_index(count, tile, n)
            total = None
            for ref, factor in zip(refs, factors):
                scale = jnp.take_along_axis(factor, index, axis=1, mode="promise_in_bounds")
                term = load(ref, part) * scale
                total = term if total is None else total + term
            if tile == wide // 128 - 1:
                total = jnp.where(is_max, top, total)
            dst[..., part] = total.reshape(*shape, 128)

    def z_of(dz):
        return lax.rem(z + dz + NZ, NZ)

    def x_of(dx):
        return lax.rem(x + dx + NX, NX)

    def send(g, n, src, dst, dz, dx):
        remote(src, dst, r_send.at[g], r_recv.at[g, n], there(dz, dx)).start()

    def receive(g, n, dst):
        remote(dst, dst, r_send.at[g], r_recv.at[g, n], there(1, 0)).wait_recv()

    def z_first(g, s):
        count, mine = GROUPS[g], own[g]
        zr, zl, xr, xl = inbox[g]
        if s <= 3:
            if s > 0:
                receive(g, s - 1, zr.at[s - 1])
                merge(count, mine.at[z_of(4 - s)], [zr.at[s - 1]])
            send(g, s, mine.at[z_of(4 - s)], zr.at[s], 1, 0)
            if s < 3:
                if s > 0:
                    receive(g, 3 + s, zl.at[s - 1])
                    merge(count, mine.at[z_of(s - 3)], [zl.at[s - 1]])
                send(g, 4 + s, mine.at[z_of(s - 3)], zl.at[s], -1, 0)
        elif s == 4:
            receive(g, 6, zl.at[2])
            receive(g, 3, zr.at[3])
            merge(count, mine.at[z], [zr.at[3], zl.at[2]])
            send(g, 7, mine.at[z, x_of(2)], xr.at[0], 0, 1)
            send(g, 9, mine.at[z, x_of(-1)], xl, 0, -1)
        elif s == 5:
            receive(g, 7, xr.at[0])
            merge(count, mine.at[z, x_of(1)], [xr.at[0]])
            send(g, 8, mine.at[z, x_of(1)], xr.at[1], 0, 1)
        else:
            receive(g, 9, xl)
            receive(g, 8, xr.at[1])
            merge(count, mine.at[z, x], [xr.at[1], xl])

    def x_first(g, s):
        count, mine = GROUPS[g], own[g]
        half, right, left, rest = inbox[g]
        low, high = pl.ds(0, NZ // 2), pl.ds(NZ // 2, NZ // 2)
        if s == 0:
            send(g, 0, mine.at[low, x_of(2)], half.at[0], 0, 1)
            send(g, 1, mine.at[high, x_of(2)], half.at[1], 0, -1)
        elif s == 1:
            receive(g, 0, half.at[0])
            merge(count, mine.at[low, x_of(1)], [half.at[0]])
            send(g, 2, mine.at[:, x_of(1)], right, 0, 1)
            receive(g, 1, half.at[1])
            merge(count, mine.at[high, x_of(-1)], [half.at[1]])
            send(g, 3, mine.at[:, x_of(-1)], left, 0, -1)
        elif s == 2:
            receive(g, 2, right)
            receive(g, 3, left)
            merge(count, mine.at[:, x], [right, left])
            for dz in (4, 3, 5, 2, 6, 1, 7):
                send(g, 4, mine.at[z_of(dz), x], rest.at[dz - 1], dz, 0)
        else:
            receive(g, 4, rest)
            merge(count, mine.at[z, x], [rest.at[k] for k in range(NZ - 1)])

    starts = [sum(GROUPS[:g]) for g in range(len(GROUPS))]

    def finish(g):
        count = GROUPS[g]
        wide = lanes(count)
        mine = own[g].at[z, x]
        inverse = 1.0 / mine[:, wide - 128 :]
        parts = []
        for tile in range(wide // 128):
            index = jnp.clip(spread_index(count, tile, 8) + count * HEADS, 0, 127)
            scale = jnp.take_along_axis(inverse, index, axis=1, mode="promise_in_bounds")
            parts.append(mine[:, tile * 128 : (tile + 1) * 128] * scale)
        mixed = jnp.concatenate(parts, axis=1)
        for u in range(count):
            mh, ml = split(mixed[:, u * width : (u + 1) * width])
            out_ref[starts[g] + u] = (
                jnp.dot(mh, woc[0], preferred_element_type=F32)
                + jnp.dot(mh, woc[1], preferred_element_type=F32)
                + jnp.dot(ml, woc[0], preferred_element_type=F32)
                + jnp.dot(ml, woc[1], preferred_element_type=F32)
            )

    def tick(g, s):
        with jax.named_scope("t%d_%d" % (g, s)):
            if s == 0:
                own[g][...] = ot[: lanes(GROUPS[g]), :].T.reshape(own[g].shape)
            (z_first if g in Z_FIRST else x_first)(g, s)
            if s == (6 if g in Z_FIRST else 3):
                finish(g)

    def att(first, last):
        group = max(g for g in range(len(GROUPS)) if starts[g] <= first)

        def body(f, c):
            attend(starts[group], GROUPS[group], f)
            return c

        with jax.named_scope("att"):
            lax.fori_loop(first, last + nothing, body, 0)

    schedule = [
        (0, 1, [(project_queries, 0)], []),
        (1, 3, [(further_x, 2), (along_x, 4), (project_queries, 1)], [(0, 0)]),
        (3, 5, [(further_x, 3), (along_x, 5), (project_queries, 2)], [(0, 1)]),
        (5, 6, [(further_x, 4), (project_queries, 3)], [(1, 0)]),
        (6, 7, [(further_x, 5)], [(0, 2)]),
        (7, 8, [(project_queries, 4)], [(2, 0), (1, 1)]),
        (8, 9, [], [(0, 3)]),
        (9, 10, [(project_queries, 5)], [(3, 0), (2, 1)]),
        (10, 11, [], [(4, 0), (1, 2), (0, 4)]),
        (11, 12, [],
         [(5, 0), (2, 2), (3, 1), (0, 5), (4, 1), (5, 1), (2, 3), (0, 6), (3, 2), (4, 2), (1, 3)]
         + [(2, 4), (5, 2), (2, 5), (3, 3), (4, 3), (2, 6), (5, 3)]),
    ]
    for first, last, before, ticks in schedule:
        for act, n in before:
            act(n)
        if first == 0:
            scores(0, 0)
        att(first, last)
        for g, s in ticks:
            tick(g, s)

    for half in range(2):
        weights_all(half).wait_send()
    for p in range(pairs):
        for n in range(3):
            stage_all(p, n).wait_send()
    for g in range(len(GROUPS)):
        sent = [own[g].at[pl.ds(0, 7)], own[g].at[0, pl.ds(0, 3)]]
        if g not in Z_FIRST:
            sent = [own[g].at[pl.ds(0, 6)], own[g].at[pl.ds(0, 7), 0]]
        for ref in sent:
            remote(ref, ref, r_send.at[g], r_recv.at[g, 0], there(1, 0)).wait_send()


def per_device(test_cells, train_cells, w_query, w_key, w_value, w_out):
    cells = jnp.transpose(train_cells, (1, 2, 0))
    tests = jnp.transpose(test_cells, (1, 0, 2))
    features, width, rows = cells.shape
    mine = tests.shape[1]
    owners = NZ * NX
    all_tests = owners * mine
    inboxes = []
    for g, count in enumerate(GROUPS):
        outer = [(4, NX), (3, NX), (2,), ()] if g in Z_FIRST else [(2, 4), (NZ,), (NZ,), (NZ - 1,)]
        inboxes.append([pltpu.VMEM((*o, mine, lanes(count)), F32) for o in outer])
    vmem = pl.BlockSpec(memory_space=pltpu.VMEM)
    dma = pltpu.SemaphoreType.DMA
    out = pl.pallas_call(
        kernel,
        out_shape=jax.ShapeDtypeStruct((features, mine, width), F32),
        in_specs=[pl.BlockSpec(memory_space=pl.ANY)] + [vmem] * 5,
        out_specs=vmem,
        scratch_shapes=[
            pltpu.VMEM((features, width, rows), F32),
            pltpu.VMEM((2, NF, width // NF, 2 * width), F32),
            pltpu.VMEM((features // 2, NZ, NX, mine, 2 * width), F32),
            pltpu.VMEM((features, HEADS, rows, 4 * HEAD), BF),
            pltpu.VMEM((features, HEADS // 2, VROWS, rows), BF),
            pltpu.VMEM((features, HEADS, 4 * HEAD, all_tests), BF),
            pltpu.VMEM((2 * width, 4 * width), BF),
            pltpu.VMEM((width, 4 * width), BF),
            pltpu.VMEM((2, width, width), BF),
            pltpu.VMEM((lanes(max(GROUPS)), all_tests), F32),
            pltpu.VMEM((2, 2 * width, rows), F32),
            pltpu.VMEM((HEADS // 2, 2, rows, all_tests), F32),
            dma((features,)),
            dma((2,)),
            dma((2,)),
            dma((features // 2, 3)),
            dma((features // 2, 3)),
            dma((len(GROUPS),)),
            dma((len(GROUPS), 10)),
            [pltpu.VMEM((NZ, NX, mine, lanes(n)), F32) for n in GROUPS],
            inboxes,
        ],
        compiler_params=pltpu.CompilerParams(
            collective_id=0, has_side_effects=True, vmem_limit_bytes=60 * 2**20
        ),
        name="attention",
    )(cells, tests, w_query, w_key, w_value, w_out)
    return jnp.transpose(out, (1, 0, 2))


def solution(mesh):
    rows = P("rows", "feat", None)
    weights = P("feat", None)
    return jax.shard_map(
        per_device,
        mesh=mesh,
        in_specs=(rows, rows, weights, weights, weights, weights),
        out_specs=rows,
        check_vma=False,
    )
```

```python
import functools

import jax
import jax.numpy as jnp
from jax import lax
from jax.experimental import pallas as pl
from jax.experimental.pallas import tpu as pltpu
from jax.sharding import PartitionSpec as P

BF = jnp.bfloat16
F32 = jnp.float32
HEADS = 6
HEAD = 32
LOG2E = 1.4426950408889634
NZ, NX, NF = 8, 4, 8
VROWS = 4 * HEAD + 16
ROW_FIRST = (4, 5)
GROUPS = (3, 3, 2, 2, 1, 1)
Z_FIRST = (0,)
MESH = pl.DeviceIdType.MESH


def split(x):
    hi = x.astype(BF)
    return hi, (x - hi.astype(F32)).astype(BF)


def lanes(count):
    return -(-count * HEADS * (HEAD + 2) // 128) * 128


def kernel(
    x_hbm, t_hbm, wq_hbm, wk_hbm, wv_hbm, wo_hbm, out_ref,
    xb, wb, gat, kp, vp, qp, wkv, wqc, woc, ot, kv, sc,
    x_sem, w_send, w_recv, g_send, g_recv, r_send, r_recv, own, inbox, t_ref, w_ref, in_sem,
):
    width = HEADS * HEAD
    features = x_hbm.shape[0]
    rows = x_hbm.shape[2]
    tests = gat.shape[1] * gat.shape[2] * gat.shape[3]
    feat, place = lax.axis_index("feat"), lax.axis_index("rows")
    z, x = place // NX, place % NX
    nothing = place // (NZ * NX)

    def at(dz, dx):
        return lax.rem(z + dz + NZ, NZ) * NX + lax.rem(x + dx + NX, NX)

    def there(dz, dx):
        return {"feat": feat, "rows": at(dz, dx)}

    def peer(k):
        return {"feat": lax.rem(feat + k, NF), "rows": place}

    barrier = pltpu.get_barrier_semaphore()
    peers = [there(dz, 0) for dz in range(1, NZ)] + [there(0, 1), there(0, -1)]
    peers += [peer(k) for k in range(1, NF)]
    for other in peers:
        pl.semaphore_signal(barrier, inc=1, device_id=other, device_id_type=MESH)

    small = [pltpu.make_async_copy(t_hbm, t_ref, in_sem.at[0])]
    for n, w_hbm in enumerate((wk_hbm, wv_hbm, wq_hbm, wo_hbm)):
        small.append(pltpu.make_async_copy(w_hbm, w_ref.at[n], in_sem.at[n + 1]))
    for copy in small:
        copy.start()
    for f in range(features):
        pltpu.make_async_copy(x_hbm.at[f], xb.at[f], x_sem.at[f]).start()
    for copy in small:
        copy.wait()
    for half in range(2):
        wb[half, feat] = jnp.concatenate([w_ref[2 * half], w_ref[2 * half + 1]], axis=1)
    pairs = features // 2
    for p in range(pairs):
        gat[p, z, x] = jnp.concatenate([t_ref[2 * p], t_ref[2 * p + 1]], axis=1)
    with jax.named_scope("bar"):
        pl.semaphore_wait(barrier, len(peers))

    def remote(src, dst, send_sem, recv_sem, device):
        return pltpu.make_async_remote_copy(
            src_ref=src,
            dst_ref=dst,
            send_sem=send_sem,
            recv_sem=recv_sem,
            device_id=device,
            device_id_type=MESH,
        )

    def weights_start(half):
        for k in range(1, NF):
            mine = wb.at[half, feat]
            remote(mine, mine, w_send.at[half], w_recv.at[half], peer(k)).start()

    def weights_all(half):
        seven = wb.at[half, pl.ds(0, NF - 1)]
        return remote(seven, seven, w_send.at[half], w_recv.at[half], peer(1))

    def stage(p, n, ref, device):
        return remote(ref, ref, g_send.at[p, n], g_recv.at[p, n], device)

    def stage_all(p, n):
        if p in ROW_FIRST:
            ref = (
                gat.at[p, 0, pl.ds(0, 2)],
                gat.at[p, 0, pl.ds(0, 1)],
                gat.at[p, pl.ds(0, 2)],
                gat.at[p, pl.ds(0, 2)],
                gat.at[p, pl.ds(0, 2)],
                gat.at[p, pl.ds(0, 1)],
            )[n]
        else:
            ref = (gat.at[p, pl.ds(0, NZ - 1), 0], gat.at[p, pl.ds(0, 4)], gat.at[p, pl.ds(0, 2)])[n]
        return stage(p, n, ref, there(1, 0))

    def by_rows(p, n):
        if n > 0:
            with jax.named_scope("r%d_%d" % (n, p)):
                stage_all(p, n - 1).wait_recv()
        if n == 0:
            for dx in (1, -1):
                stage(p, 0, gat.at[p, z, x], there(0, dx)).start()
        elif n == 1:
            dx = 1 if p % 4 == 1 else -1
            stage(p, 1, gat.at[p, z, column_of(-dx)], there(0, dx)).start()
        elif n < 5:
            for dz in (1, -1):
                row = lax.rem(z - dz * (n - 2) + NZ, NZ)
                stage(p, n, gat.at[p, row], there(dz, 0)).start()
        else:
            for dz, part in ((1, 0), (-1, NX // 2)):
                row = lax.rem(z - dz * 3 + NZ, NZ)
                stage(p, n, gat.at[p, row, pl.ds(part, NX // 2)], there(dz, 0)).start()

    def column_of(dx):
        return lax.rem(x + dx + NX, NX)

    def along_z(p):
        for dz in (4, 3, 5, 2, 6, 1, 7):
            stage(p, 0, gat.at[p, z, x], there(dz, 0)).start()

    def along_x(p):
        with jax.named_scope("x1_%d" % p):
            stage_all(p, 0).wait_recv()
        for dx in (1, -1):
            stage(p, 1, gat.at[p, :, x], there(0, dx)).start()

    def further_x(p):
        with jax.named_scope("x2_%d" % p):
            stage_all(p, 1).wait_recv()
        half = NZ // 2
        stage(p, 2, gat.at[p, pl.ds(0, half), column_of(-1)], there(0, 1)).start()
        stage(p, 2, gat.at[p, pl.ds(half, half), column_of(1)], there(0, -1)).start()

    def arrived(p):
        with jax.named_scope("x3_%d" % p):
            stage_all(p, 5 if p in ROW_FIRST else 2).wait_recv()

    along_z(0)
    weights_start(0)
    for p in ROW_FIRST:
        by_rows(p, 0)
    for p in range(1, 4):
        along_z(p)
    for p in ROW_FIRST:
        by_rows(p, 1)
    along_x(0)
    for p in ROW_FIRST:
        by_rows(p, 2)
    with jax.named_scope("w0"):
        weights_all(0).wait_recv()
    weights_start(1)
    hi, lo = split(wb[0].reshape(width, 2 * width).T)
    wkv[...] = jnp.concatenate([hi, lo, hi, lo], axis=1)

    def project(f, slot):
        xh, xl_ = split(xb[f])
        kv[slot] = jnp.dot(
            wkv[...],
            jnp.concatenate([xh, xh, xl_, xl_], axis=0),
            preferred_element_type=F32,
        )

    def pack(f, slot):
        kh, kl = split(kv[slot, :width])
        vh, vl = split(kv[slot, width:])
        for h in range(HEADS):
            s = slice(h * HEAD, (h + 1) * HEAD)
            kp[f, h] = jnp.concatenate([kh[s], kh[s], kl[s], kl[s]], axis=0).T
        for g in range(HEADS // 2):
            a = slice(2 * g * HEAD, (2 * g + 1) * HEAD)
            b = slice((2 * g + 1) * HEAD, (2 * g + 2) * HEAD)
            vp[f, g] = jnp.concatenate([vh[a], vl[a], vh[b], vl[b], jnp.ones((16, rows), BF)], axis=0)

    def keys_values(p, c):
        f = 2 * p
        project(f + 1, 1)
        pack(f, 0)
        project(jnp.minimum(f + 2, features - 1), 0)
        pack(f + 1, 1)
        return c

    for f in range(features):
        pltpu.make_async_copy(x_hbm.at[f], xb.at[f], x_sem.at[f]).wait()
    project(0, 0)
    moves = [
        [(along_x, 1)],
        [],
        [(further_x, 0), (along_x, 2)],
        [],
        [],
        [(further_x, 1), (along_x, 3)],
    ]
    for p in range(pairs):
        with jax.named_scope("kv"):
            lax.fori_loop(p, p + 1 + nothing, keys_values, 0)
        for move, *n in moves[p]:
            move(*n)

    with jax.named_scope("w1"):
        weights_all(1).wait_recv()
    wt = wb[1].reshape(width, 2 * width)
    hi, lo = split(wt[:, :width].T)
    wqc[...] = jnp.concatenate([hi, lo, hi, lo], axis=1)
    hi, lo = split(wt[:, width:])
    woc[0] = hi
    woc[1] = lo

    def project_queries(p):
        arrived(p)
        queries_of(p)

    def queries_of(p):
        both = gat[p].reshape(tests, 2 * width).T
        for u in range(2):
            th, tl = split(both[u * width : (u + 1) * width])
            q = jnp.dot(
                wqc[...], jnp.concatenate([th, th, tl, tl], axis=0), preferred_element_type=F32
            ) * (HEAD**-0.5 * LOG2E)
            qh, ql = split(q)
            for h in range(HEADS):
                s = slice(h * HEAD, (h + 1) * HEAD)
                qp[2 * p + u, h] = jnp.concatenate([qh[s], ql[s], qh[s], ql[s]], axis=0)

    def scores(f, g):
        for u in range(2):
            h = 2 * g + u
            sc[g, u] = jnp.dot(kp[f, h], qp[f, h], preferred_element_type=F32)

    def attend(first, count, f):
        place_of = pl.multiple_of((f - first) * width, 8)
        stat = count * width + (f - first) * HEADS
        following = jnp.minimum(f + 1, features - 1)
        pairs_of_heads = HEADS // 2
        for g in range(pairs_of_heads):
            if g + 1 < pairs_of_heads:
                scores(f, g + 1)
            else:
                scores(following, 0)
            tops = [jnp.max(sc[g, u], axis=0, keepdims=True) for u in range(2)]
            probs = [split(jnp.exp2(sc[g, u] - tops[u])) for u in range(2)]
            both = [jnp.concatenate([p[part] for p in probs], axis=1) for part in range(2)]
            vv = vp[f, g]
            o = jnp.dot(
                jnp.concatenate([vv, vv], axis=1),
                jnp.concatenate(both, axis=0),
                preferred_element_type=F32,
            )
            for u in range(2):
                part = o[2 * u * HEAD : (2 * u + 2) * HEAD, u * tests : (u + 1) * tests]
                h = 2 * g + u
                ot[pl.ds(place_of + h * HEAD, HEAD), :] = part[:HEAD] + part[HEAD:]
                ot[pl.ds(stat + h, 1), :] = tops[u]
                ot[pl.ds(stat + count * HEADS + h, 1), :] = o[
                    4 * HEAD : 4 * HEAD + 1, u * tests : (u + 1) * tests
                ]

    def spread_index(count, tile, n):
        lane = lax.broadcasted_iota(jnp.int32, (n, 128), 1)
        wide = lanes(count)
        first = count * width - (wide - 128)
        low = first + (lane + tile * 128) // HEAD
        if tile < wide // 128 - 1:
            return low
        high = lane - count * HEADS
        return jnp.clip(jnp.where(lane < first, low, high), 0, 127)

    def merge(count, dst, srcs):
        wide = lanes(count)
        first = count * width - (wide - 128)
        shape = dst.shape[:-1]
        n = dst.size // wide
        tail = pl.ds(wide - 128, 128)

        def load(ref, part):
            return ref[..., part].reshape(n, 128)

        refs = (dst, *srcs)
        stats = [load(r, tail) for r in refs]
        top = functools.reduce(jnp.maximum, stats)
        factors = [jnp.exp2(v - top) for v in stats]
        lane = lax.broadcasted_iota(jnp.int32, (n, 128), 1)
        is_max = (lane >= first) & (lane < first + count * HEADS)
        for tile in range(wide // 128):
            part = pl.ds(tile * 128, 128)
            index = spread_index(count, tile, n)
            total = None
            for ref, factor in zip(refs, factors):
                scale = jnp.take_along_axis(factor, index, axis=1, mode="promise_in_bounds")
                term = load(ref, part) * scale
                total = term if total is None else total + term
            if tile == wide // 128 - 1:
                total = jnp.where(is_max, top, total)
            dst[..., part] = total.reshape(*shape, 128)

    def z_of(dz):
        return lax.rem(z + dz + NZ, NZ)

    def x_of(dx):
        return lax.rem(x + dx + NX, NX)

    def send(g, n, src, dst, dz, dx):
        remote(src, dst, r_send.at[g], r_recv.at[g, n], there(dz, dx)).start()

    def receive(g, n, dst):
        remote(dst, dst, r_send.at[g], r_recv.at[g, n], there(1, 0)).wait_recv()

    def z_first(g, s):
        count, mine = GROUPS[g], own[g]
        zr, zl, xr, xl = inbox[g]
        if s <= 3:
            if s > 0:
                receive(g, s - 1, zr.at[s - 1])
                merge(count, mine.at[z_of(4 - s)], [zr.at[s - 1]])
            send(g, s, mine.at[z_of(4 - s)], zr.at[s], 1, 0)
            if s < 3:
                if s > 0:
                    receive(g, 3 + s, zl.at[s - 1])
                    merge(count, mine.at[z_of(s - 3)], [zl.at[s - 1]])
                send(g, 4 + s, mine.at[z_of(s - 3)], zl.at[s], -1, 0)
        elif s == 4:
            receive(g, 6, zl.at[2])
            receive(g, 3, zr.at[3])
            merge(count, mine.at[z], [zr.at[3], zl.at[2]])
            send(g, 7, mine.at[z, x_of(2)], xr.at[0], 0, 1)
            send(g, 9, mine.at[z, x_of(-1)], xl, 0, -1)
        elif s == 5:
            receive(g, 7, xr.at[0])
            merge(count, mine.at[z, x_of(1)], [xr.at[0]])
            send(g, 8, mine.at[z, x_of(1)], xr.at[1], 0, 1)
        else:
            receive(g, 9, xl)
            receive(g, 8, xr.at[1])
            merge(count, mine.at[z, x], [xr.at[1], xl])

    def x_first(g, s):
        count, mine = GROUPS[g], own[g]
        half, right, left, rest = inbox[g]
        low, high = pl.ds(0, NZ // 2), pl.ds(NZ // 2, NZ // 2)
        if s == 0:
            send(g, 0, mine.at[low, x_of(2)], half.at[0], 0, 1)
            send(g, 1, mine.at[high, x_of(2)], half.at[1], 0, -1)
        elif s == 1:
            receive(g, 0, half.at[0])
            merge(count, mine.at[low, x_of(1)], [half.at[0]])
            send(g, 2, mine.at[:, x_of(1)], right, 0, 1)
            receive(g, 1, half.at[1])
            merge(count, mine.at[high, x_of(-1)], [half.at[1]])
            send(g, 3, mine.at[:, x_of(-1)], left, 0, -1)
        elif s == 2:
            receive(g, 2, right)
            receive(g, 3, left)
            merge(count, mine.at[:, x], [right, left])
            for dz in (4, 3, 5, 2, 6, 1, 7):
                send(g, 4, mine.at[z_of(dz), x], rest.at[dz - 1], dz, 0)
        else:
            receive(g, 4, rest)
            merge(count, mine.at[z, x], [rest.at[k] for k in range(NZ - 1)])

    starts = [sum(GROUPS[:g]) for g in range(len(GROUPS))]

    def finish(g):
        count = GROUPS[g]
        wide = lanes(count)
        mine = own[g].at[z, x]
        inverse = 1.0 / mine[:, wide - 128 :]
        parts = []
        for tile in range(wide // 128):
            index = jnp.clip(spread_index(count, tile, 8) + count * HEADS, 0, 127)
            scale = jnp.take_along_axis(inverse, index, axis=1, mode="promise_in_bounds")
            parts.append(mine[:, tile * 128 : (tile + 1) * 128] * scale)
        mixed = jnp.concatenate(parts, axis=1)
        for u in range(count):
            mh, ml = split(mixed[:, u * width : (u + 1) * width])
            out_ref[starts[g] + u] = (
                jnp.dot(mh, woc[0], preferred_element_type=F32)
                + jnp.dot(mh, woc[1], preferred_element_type=F32)
                + jnp.dot(ml, woc[0], preferred_element_type=F32)
                + jnp.dot(ml, woc[1], preferred_element_type=F32)
            )

    def tick(g, s):
        with jax.named_scope("t%d_%d" % (g, s)):
            if s == 0:
                own[g][...] = ot[: lanes(GROUPS[g]), :].T.reshape(own[g].shape)
            (z_first if g in Z_FIRST else x_first)(g, s)
            if s == (6 if g in Z_FIRST else 3):
                finish(g)

    def att(first, last, ahead):
        group = max(g for g in range(len(GROUPS)) if starts[g] <= first)

        def body(f, c):
            if ahead is not None:
                queries_of(ahead)
            attend(starts[group], GROUPS[group], f)
            return c

        with jax.named_scope("att"):
            lax.fori_loop(first, last + nothing, body, 0)

    schedule = [
        (0, 1, None, [(project_queries, 0), (by_rows, 4, 3), (by_rows, 5, 3)], []),
        (1, 3, None, [(further_x, 2), (project_queries, 1)], [(0, 0)]),
        (3, 4, 2, [(further_x, 3), (by_rows, 4, 4), (by_rows, 5, 4), (arrived, 2)], []),
        (4, 5, None, [], [(0, 1), (by_rows, 4, 5)]),
        (5, 6, 3, [(arrived, 3)], [(1, 0), (by_rows, 5, 5)]),
        (6, 7, None, [], [(0, 2)]),
        (7, 8, 4, [(arrived, 4)], [(2, 0), (1, 1)]),
        (8, 9, None, [], [(0, 3)]),
        (9, 10, 5, [(arrived, 5)], [(3, 0)]),
        (10, 11, None, [], [(4, 0), (2, 1), (0, 4)]),
        (11, 12, None, [],
         [(5, 0), (1, 2), (3, 1), (4, 1), (0, 5), (2, 2), (5, 1), (3, 2), (1, 3), (4, 2)]
         + [(0, 6), (5, 2), (2, 3), (3, 3), (4, 3), (5, 3)]),
    ]
    for first, last, ahead, before, ticks in schedule:
        for act, *n in before:
            act(*n)
        if first == 0:
            scores(0, 0)
        att(first, last, ahead)
        for act in ticks:
            if len(act) == 2:
                tick(*act)
            else:
                act[0](*act[1:])

    for half in range(2):
        weights_all(half).wait_send()
    for p in range(pairs):
        for n in range(6 if p in ROW_FIRST else 3):
            stage_all(p, n).wait_send()
    for g in range(len(GROUPS)):
        sent = [own[g].at[pl.ds(0, 7)], own[g].at[0, pl.ds(0, 3)]]
        if g not in Z_FIRST:
            sent = [own[g].at[pl.ds(0, 6)], own[g].at[pl.ds(0, 7), 0]]
        for ref in sent:
            remote(ref, ref, r_send.at[g], r_recv.at[g, 0], there(1, 0)).wait_send()


def per_device(test_cells, train_cells, w_query, w_key, w_value, w_out):
    cells = jnp.transpose(train_cells, (1, 2, 0))
    tests = jnp.transpose(test_cells, (1, 0, 2))
    features, width, rows = cells.shape
    mine = tests.shape[1]
    owners = NZ * NX
    all_tests = owners * mine
    inboxes = []
    for g, count in enumerate(GROUPS):
        outer = [(4, NX), (3, NX), (2,), ()] if g in Z_FIRST else [(2, 4), (NZ,), (NZ,), (NZ - 1,)]
        inboxes.append([pltpu.VMEM((*o, mine, lanes(count)), F32) for o in outer])
    vmem = pl.BlockSpec(memory_space=pltpu.VMEM)
    dma = pltpu.SemaphoreType.DMA
    out = pl.pallas_call(
        kernel,
        out_shape=pltpu.VMEM((features, mine, width), F32),
        in_specs=[pl.BlockSpec(memory_space=pl.ANY)] * 6,
        out_specs=pl.BlockSpec(memory_space=pltpu.VMEM),
        scratch_shapes=[
            pltpu.VMEM((features, width, rows), F32),
            pltpu.VMEM((2, NF, width // NF, 2 * width), F32),
            pltpu.VMEM((features // 2, NZ, NX, mine, 2 * width), F32),
            pltpu.VMEM((features, HEADS, rows, 4 * HEAD), BF),
            pltpu.VMEM((features, HEADS // 2, VROWS, rows), BF),
            pltpu.VMEM((features, HEADS, 4 * HEAD, all_tests), BF),
            pltpu.VMEM((2 * width, 4 * width), BF),
            pltpu.VMEM((width, 4 * width), BF),
            pltpu.VMEM((2, width, width), BF),
            pltpu.VMEM((lanes(max(GROUPS)), all_tests), F32),
            pltpu.VMEM((2, 2 * width, rows), F32),
            pltpu.VMEM((HEADS // 2, 2, rows, all_tests), F32),
            dma((features,)),
            dma((2,)),
            dma((2,)),
            dma((features // 2, 6)),
            dma((features // 2, 6)),
            dma((len(GROUPS),)),
            dma((len(GROUPS), 10)),
            [pltpu.VMEM((NZ, NX, mine, lanes(n)), F32) for n in GROUPS],
            inboxes,
            pltpu.VMEM((features, mine, width), F32),
            pltpu.VMEM((4, width // NF, width), F32),
            dma((5,)),
        ],
        compiler_params=pltpu.CompilerParams(
            collective_id=0, has_side_effects=True, vmem_limit_bytes=60 * 2**20
        ),
        name="attention",
    )(cells, tests, w_query, w_key, w_value, w_out)
    return jnp.transpose(out, (1, 0, 2))


def solution(mesh):
    rows = P("rows", "feat", None)
    weights = P("feat", None)
    return jax.shard_map(
        per_device,
        mesh=mesh,
        in_specs=(rows, rows, weights, weights, weights, weights),
        out_specs=rows,
        check_vma=False,
    )
```

```python
import functools

import jax
import jax.numpy as jnp
from jax import lax
from jax.experimental import pallas as pl
from jax.experimental.pallas import tpu as pltpu
from jax.sharding import PartitionSpec as P

BF = jnp.bfloat16
F32 = jnp.float32
HEADS = 6
HEAD = 32
LOG2E = 1.4426950408889634
NZ, NX, NF = 8, 4, 8
VROWS = 4 * HEAD + 16
ROW_FIRST = (4, 5)
GROUPS = (3, 3, 2, 2, 1, 1)
Z_FIRST = (0,)
MESH = pl.DeviceIdType.MESH


def split(x):
    hi = x.astype(BF)
    return hi, (x - hi.astype(F32)).astype(BF)


def lanes(count):
    return -(-count * HEADS * (HEAD + 2) // 128) * 128


def kernel(
    x_hbm, t_hbm, wq_hbm, wk_hbm, wv_hbm, wo_hbm, out_ref,
    xb, wb, gat, kp, vp, qp, wkv, wqc, woc, ot, kv, sc,
    x_sem, w_send, w_recv, g_send, g_recv, r_send, r_recv, own, inbox, t_ref, w_ref, in_sem,
):
    width = HEADS * HEAD
    features = x_hbm.shape[0]
    rows = x_hbm.shape[2]
    tests = gat.shape[1] * gat.shape[2] * gat.shape[3]
    feat, place = lax.axis_index("feat"), lax.axis_index("rows")
    z, x = place // NX, place % NX
    nothing = place // (NZ * NX)

    def at(dz, dx):
        return lax.rem(z + dz + NZ, NZ) * NX + lax.rem(x + dx + NX, NX)

    def there(dz, dx):
        return {"feat": feat, "rows": at(dz, dx)}

    def peer(k):
        return {"feat": lax.rem(feat + k, NF), "rows": place}

    barrier = pltpu.get_barrier_semaphore()
    peers = [there(dz, 0) for dz in range(1, NZ)] + [there(0, 1), there(0, -1)]
    peers += [peer(k) for k in range(1, NF)]
    for other in peers:
        pl.semaphore_signal(barrier, inc=1, device_id=other, device_id_type=MESH)

    small = [pltpu.make_async_copy(t_hbm, t_ref, in_sem.at[0])]
    for n, w_hbm in enumerate((wk_hbm, wv_hbm, wq_hbm, wo_hbm)):
        small.append(pltpu.make_async_copy(w_hbm, w_ref.at[n], in_sem.at[n + 1]))
    for copy in small:
        copy.start()
    for f in range(features):
        pltpu.make_async_copy(x_hbm.at[f], xb.at[f], x_sem.at[f]).start()
    for copy in small:
        copy.wait()
    for half in range(2):
        wb[half, feat] = jnp.concatenate([w_ref[2 * half], w_ref[2 * half + 1]], axis=1)
    pairs = features // 2
    for p in range(pairs):
        gat[p, z, x] = jnp.concatenate([t_ref[2 * p], t_ref[2 * p + 1]], axis=1)
    with jax.named_scope("bar"):
        pl.semaphore_wait(barrier, len(peers))

    def remote(src, dst, send_sem, recv_sem, device):
        return pltpu.make_async_remote_copy(
            src_ref=src,
            dst_ref=dst,
            send_sem=send_sem,
            recv_sem=recv_sem,
            device_id=device,
            device_id_type=MESH,
        )

    def weights_start(half):
        for k in range(1, NF):
            mine = wb.at[half, feat]
            remote(mine, mine, w_send.at[half], w_recv.at[half], peer(k)).start()

    def weights_all(half):
        seven = wb.at[half, pl.ds(0, NF - 1)]
        return remote(seven, seven, w_send.at[half], w_recv.at[half], peer(1))

    def stage(p, n, ref, device):
        return remote(ref, ref, g_send.at[p, n], g_recv.at[p, n], device)

    def stage_all(p, n):
        if p in ROW_FIRST:
            ref = (
                gat.at[p, 0, pl.ds(0, 2)],
                gat.at[p, 0, pl.ds(0, 1)],
                gat.at[p, pl.ds(0, 2)],
                gat.at[p, pl.ds(0, 2)],
                gat.at[p, pl.ds(0, 2)],
                gat.at[p, pl.ds(0, 1)],
            )[n]
        else:
            ref = (gat.at[p, pl.ds(0, NZ - 1), 0], gat.at[p, pl.ds(0, 4)], gat.at[p, pl.ds(0, 2)])[n]
        return stage(p, n, ref, there(1, 0))

    def by_rows(p, n):
        if n > 0:
            with jax.named_scope("r%d_%d" % (n, p)):
                stage_all(p, n - 1).wait_recv()
        if n == 0:
            for dx in (1, -1):
                stage(p, 0, gat.at[p, z, x], there(0, dx)).start()
        elif n == 1:
            dx = 1 if p % 4 == 1 else -1
            stage(p, 1, gat.at[p, z, column_of(-dx)], there(0, dx)).start()
        elif n < 5:
            for dz in (1, -1):
                row = lax.rem(z - dz * (n - 2) + NZ, NZ)
                stage(p, n, gat.at[p, row], there(dz, 0)).start()
        else:
            for dz, part in ((1, 0), (-1, NX // 2)):
                row = lax.rem(z - dz * 3 + NZ, NZ)
                stage(p, n, gat.at[p, row, pl.ds(part, NX // 2)], there(dz, 0)).start()

    def column_of(dx):
        return lax.rem(x + dx + NX, NX)

    def along_z(p):
        for dz in (4, 3, 5, 2, 6, 1, 7):
            stage(p, 0, gat.at[p, z, x], there(dz, 0)).start()

    def along_x(p):
        with jax.named_scope("x1_%d" % p):
            stage_all(p, 0).wait_recv()
        for dx in (1, -1):
            stage(p, 1, gat.at[p, :, x], there(0, dx)).start()

    def further_x(p):
        with jax.named_scope("x2_%d" % p):
            stage_all(p, 1).wait_recv()
        half = NZ // 2
        stage(p, 2, gat.at[p, pl.ds(0, half), column_of(-1)], there(0, 1)).start()
        stage(p, 2, gat.at[p, pl.ds(half, half), column_of(1)], there(0, -1)).start()

    def arrived(p):
        with jax.named_scope("x3_%d" % p):
            stage_all(p, 5 if p in ROW_FIRST else 2).wait_recv()

    along_z(0)
    weights_start(0)
    for p in ROW_FIRST:
        by_rows(p, 0)
    for p in range(1, 4):
        along_z(p)
    for p in ROW_FIRST:
        by_rows(p, 1)
    along_x(0)
    for p in ROW_FIRST:
        by_rows(p, 2)
    with jax.named_scope("w0"):
        weights_all(0).wait_recv()
    weights_start(1)
    hi, lo = split(wb[0].reshape(width, 2 * width).T)
    wkv[...] = jnp.concatenate([hi, lo, hi, lo], axis=1)

    def project(f, slot):
        xh, xl_ = split(xb[f])
        kv[slot] = jnp.dot(
            wkv[...],
            jnp.concatenate([xh, xh, xl_, xl_], axis=0),
            preferred_element_type=F32,
        )

    def pack(f, slot):
        kh, kl = split(kv[slot, :width])
        vh, vl = split(kv[slot, width:])
        for h in range(HEADS):
            s = slice(h * HEAD, (h + 1) * HEAD)
            kp[f, h] = jnp.concatenate([kh[s], kh[s], kl[s], kl[s]], axis=0).T
        for g in range(HEADS // 2):
            a = slice(2 * g * HEAD, (2 * g + 1) * HEAD)
            b = slice((2 * g + 1) * HEAD, (2 * g + 2) * HEAD)
            vp[f, g] = jnp.concatenate([vh[a], vl[a], vh[b], vl[b], jnp.ones((16, rows), BF)], axis=0)

    def keys_values(p, c):
        f = 2 * p
        project(f + 1, 1)
        pack(f, 0)
        project(jnp.minimum(f + 2, features - 1), 0)
        pack(f + 1, 1)
        return c

    for f in range(features):
        pltpu.make_async_copy(x_hbm.at[f], xb.at[f], x_sem.at[f]).wait()
    project(0, 0)
    moves = [
        [(along_x, 1)],
        [],
        [(further_x, 0), (along_x, 2)],
        [(by_rows, 4, 3), (by_rows, 5, 3)],
        [],
        [(further_x, 1), (along_x, 3)],
    ]
    for p in range(pairs):
        with jax.named_scope("kv"):
            lax.fori_loop(p, p + 1 + nothing, keys_values, 0)
        for move, *n in moves[p]:
            move(*n)

    with jax.named_scope("w1"):
        weights_all(1).wait_recv()
    wt = wb[1].reshape(width, 2 * width)
    hi, lo = split(wt[:, :width].T)
    wqc[...] = jnp.concatenate([hi, lo, hi, lo], axis=1)
    hi, lo = split(wt[:, width:])
    woc[0] = hi
    woc[1] = lo

    def project_queries(p):
        arrived(p)
        queries_of(p)

    def queries_of(p):
        both = gat[p].reshape(tests, 2 * width).T
        for u in range(2):
            th, tl = split(both[u * width : (u + 1) * width])
            q = jnp.dot(
                wqc[...], jnp.concatenate([th, th, tl, tl], axis=0), preferred_element_type=F32
            ) * (HEAD**-0.5 * LOG2E)
            qh, ql = split(q)
            for h in range(HEADS):
                s = slice(h * HEAD, (h + 1) * HEAD)
                qp[2 * p + u, h] = jnp.concatenate([qh[s], ql[s], qh[s], ql[s]], axis=0)

    def scores(f, g):
        for u in range(2):
            h = 2 * g + u
            sc[g, u] = jnp.dot(kp[f, h], qp[f, h], preferred_element_type=F32)

    def attend(first, count, f):
        place_of = pl.multiple_of((f - first) * width, 8)
        stat = count * width + (f - first) * HEADS
        following = jnp.minimum(f + 1, features - 1)
        pairs_of_heads = HEADS // 2
        for g in range(pairs_of_heads):
            if g + 1 < pairs_of_heads:
                scores(f, g + 1)
            else:
                scores(following, 0)
            tops = [jnp.max(sc[g, u], axis=0, keepdims=True) for u in range(2)]
            probs = [split(jnp.exp2(sc[g, u] - tops[u])) for u in range(2)]
            both = [jnp.concatenate([p[part] for p in probs], axis=1) for part in range(2)]
            vv = vp[f, g]
            o = jnp.dot(
                jnp.concatenate([vv, vv], axis=1),
                jnp.concatenate(both, axis=0),
                preferred_element_type=F32,
            )
            for u in range(2):
                part = o[2 * u * HEAD : (2 * u + 2) * HEAD, u * tests : (u + 1) * tests]
                h = 2 * g + u
                ot[pl.ds(place_of + h * HEAD, HEAD), :] = part[:HEAD] + part[HEAD:]
                ot[pl.ds(stat + h, 1), :] = tops[u]
                ot[pl.ds(stat + count * HEADS + h, 1), :] = o[
                    4 * HEAD : 4 * HEAD + 1, u * tests : (u + 1) * tests
                ]

    def spread_index(count, tile, n):
        lane = lax.broadcasted_iota(jnp.int32, (n, 128), 1)
        wide = lanes(count)
        first = count * width - (wide - 128)
        low = first + (lane + tile * 128) // HEAD
        if tile < wide // 128 - 1:
            return low
        high = lane - count * HEADS
        return jnp.clip(jnp.where(lane < first, low, high), 0, 127)

    def merge(count, dst, srcs):
        wide = lanes(count)
        first = count * width - (wide - 128)
        shape = dst.shape[:-1]
        n = dst.size // wide
        tail = pl.ds(wide - 128, 128)

        def load(ref, part):
            return ref[..., part].reshape(n, 128)

        refs = (dst, *srcs)
        stats = [load(r, tail) for r in refs]
        top = functools.reduce(jnp.maximum, stats)
        factors = [jnp.exp2(v - top) for v in stats]
        lane = lax.broadcasted_iota(jnp.int32, (n, 128), 1)
        is_max = (lane >= first) & (lane < first + count * HEADS)
        for tile in range(wide // 128):
            part = pl.ds(tile * 128, 128)
            index = spread_index(count, tile, n)
            total = None
            for ref, factor in zip(refs, factors):
                scale = jnp.take_along_axis(factor, index, axis=1, mode="promise_in_bounds")
                term = load(ref, part) * scale
                total = term if total is None else total + term
            if tile == wide // 128 - 1:
                total = jnp.where(is_max, top, total)
            dst[..., part] = total.reshape(*shape, 128)

    def z_of(dz):
        return lax.rem(z + dz + NZ, NZ)

    def x_of(dx):
        return lax.rem(x + dx + NX, NX)

    def send(g, n, src, dst, dz, dx):
        remote(src, dst, r_send.at[g], r_recv.at[g, n], there(dz, dx)).start()

    def receive(g, n, dst):
        remote(dst, dst, r_send.at[g], r_recv.at[g, n], there(1, 0)).wait_recv()

    def z_first(g, s):
        count, mine = GROUPS[g], own[g]
        zr, zl, xr, xl = inbox[g]
        if s <= 3:
            if s > 0:
                receive(g, s - 1, zr.at[s - 1])
                merge(count, mine.at[z_of(4 - s)], [zr.at[s - 1]])
            send(g, s, mine.at[z_of(4 - s)], zr.at[s], 1, 0)
            if s < 3:
                if s > 0:
                    receive(g, 3 + s, zl.at[s - 1])
                    merge(count, mine.at[z_of(s - 3)], [zl.at[s - 1]])
                send(g, 4 + s, mine.at[z_of(s - 3)], zl.at[s], -1, 0)
        elif s == 4:
            receive(g, 6, zl.at[2])
            receive(g, 3, zr.at[3])
            merge(count, mine.at[z], [zr.at[3], zl.at[2]])
            send(g, 7, mine.at[z, x_of(2)], xr.at[0], 0, 1)
            send(g, 9, mine.at[z, x_of(-1)], xl, 0, -1)
        elif s == 5:
            receive(g, 7, xr.at[0])
            merge(count, mine.at[z, x_of(1)], [xr.at[0]])
            send(g, 8, mine.at[z, x_of(1)], xr.at[1], 0, 1)
        else:
            receive(g, 9, xl)
            receive(g, 8, xr.at[1])
            merge(count, mine.at[z, x], [xr.at[1], xl])

    def x_first(g, s):
        count, mine = GROUPS[g], own[g]
        half, right, left, rest = inbox[g]
        low, high = pl.ds(0, NZ // 2), pl.ds(NZ // 2, NZ // 2)
        if s == 0:
            send(g, 0, mine.at[low, x_of(2)], half.at[0], 0, 1)
            send(g, 1, mine.at[high, x_of(2)], half.at[1], 0, -1)
        elif s == 1:
            receive(g, 0, half.at[0])
            merge(count, mine.at[low, x_of(1)], [half.at[0]])
            send(g, 2, mine.at[:, x_of(1)], right, 0, 1)
            receive(g, 1, half.at[1])
            merge(count, mine.at[high, x_of(-1)], [half.at[1]])
            send(g, 3, mine.at[:, x_of(-1)], left, 0, -1)
        elif s == 2:
            receive(g, 2, right)
            receive(g, 3, left)
            merge(count, mine.at[:, x], [right, left])
            for dz in (4, 3, 5, 2, 6, 1, 7):
                send(g, 4, mine.at[z_of(dz), x], rest.at[dz - 1], dz, 0)
        else:
            receive(g, 4, rest)
            merge(count, mine.at[z, x], [rest.at[k] for k in range(NZ - 1)])

    starts = [sum(GROUPS[:g]) for g in range(len(GROUPS))]

    def finish(g):
        count = GROUPS[g]
        wide = lanes(count)
        mine = own[g].at[z, x]
        inverse = 1.0 / mine[:, wide - 128 :]
        parts = []
        for tile in range(wide // 128):
            index = jnp.clip(spread_index(count, tile, 8) + count * HEADS, 0, 127)
            scale = jnp.take_along_axis(inverse, index, axis=1, mode="promise_in_bounds")
            parts.append(mine[:, tile * 128 : (tile + 1) * 128] * scale)
        mixed = jnp.concatenate(parts, axis=1)
        for u in range(count):
            mh, ml = split(mixed[:, u * width : (u + 1) * width])
            out_ref[starts[g] + u] = (
                jnp.dot(mh, woc[0], preferred_element_type=F32)
                + jnp.dot(mh, woc[1], preferred_element_type=F32)
                + jnp.dot(ml, woc[0], preferred_element_type=F32)
                + jnp.dot(ml, woc[1], preferred_element_type=F32)
            )

    def tick(g, s):
        with jax.named_scope("t%d_%d" % (g, s)):
            if s == 0:
                own[g][...] = ot[: lanes(GROUPS[g]), :].T.reshape(own[g].shape)
            (z_first if g in Z_FIRST else x_first)(g, s)
            if s == (6 if g in Z_FIRST else 3):
                finish(g)

    def att(first, last, ahead):
        group = max(g for g in range(len(GROUPS)) if starts[g] <= first)

        def body(f, c):
            if ahead is not None:
                queries_of(ahead)
            attend(starts[group], GROUPS[group], f)
            return c

        with jax.named_scope("att"):
            lax.fori_loop(first, last + nothing, body, 0)

    schedule = [
        (0, 1, None, [(project_queries, 0)], []),
        (1, 3, None, [(further_x, 2), (by_rows, 4, 4), (by_rows, 5, 4), (project_queries, 1)],
         [(0, 0), (by_rows, 4, 5), (by_rows, 5, 5)]),
        (3, 4, 2, [(further_x, 3), (arrived, 2)], []),
        (4, 5, None, [], []),
        (5, 6, 3, [(arrived, 3)], [(1, 0), (0, 1)]),
        (6, 7, None, [], []),
        (7, 8, 4, [(arrived, 4)], [(2, 0), (1, 1), (0, 2)]),
        (8, 9, None, [], []),
        (9, 10, 5, [(arrived, 5)], [(3, 0), (2, 1)]),
        (10, 11, None, [], [(4, 0), (0, 3)]),
        (11, 12, None, [],
         [(5, 0), (1, 2), (3, 1), (2, 2), (4, 1), (5, 1), (0, 4), (3, 2), (4, 2), (5, 2)]
         + [(1, 3), (0, 5), (2, 3), (0, 6), (3, 3), (4, 3), (5, 3)]),
    ]
    for first, last, ahead, before, ticks in schedule:
        for act, *n in before:
            act(*n)
        if first == 0:
            scores(0, 0)
        att(first, last, ahead)
        for act in ticks:
            if len(act) == 2:
                tick(*act)
            else:
                act[0](*act[1:])

    for half in range(2):
        weights_all(half).wait_send()
    for p in range(pairs):
        for n in range(6 if p in ROW_FIRST else 3):
            stage_all(p, n).wait_send()
    for g in range(len(GROUPS)):
        sent = [own[g].at[pl.ds(0, 7)], own[g].at[0, pl.ds(0, 3)]]
        if g not in Z_FIRST:
            sent = [own[g].at[pl.ds(0, 6)], own[g].at[pl.ds(0, 7), 0]]
        for ref in sent:
            remote(ref, ref, r_send.at[g], r_recv.at[g, 0], there(1, 0)).wait_send()


def per_device(test_cells, train_cells, w_query, w_key, w_value, w_out):
    cells = jnp.transpose(train_cells, (1, 2, 0))
    tests = jnp.transpose(test_cells, (1, 0, 2))
    features, width, rows = cells.shape
    mine = tests.shape[1]
    owners = NZ * NX
    all_tests = owners * mine
    inboxes = []
    for g, count in enumerate(GROUPS):
        outer = [(4, NX), (3, NX), (2,), ()] if g in Z_FIRST else [(2, 4), (NZ,), (NZ,), (NZ - 1,)]
        inboxes.append([pltpu.VMEM((*o, mine, lanes(count)), F32) for o in outer])
    vmem = pl.BlockSpec(memory_space=pltpu.VMEM)
    dma = pltpu.SemaphoreType.DMA
    out = pl.pallas_call(
        kernel,
        out_shape=pltpu.VMEM((features, mine, width), F32),
        in_specs=[pl.BlockSpec(memory_space=pl.ANY)] * 6,
        out_specs=pl.BlockSpec(memory_space=pltpu.VMEM),
        scratch_shapes=[
            pltpu.VMEM((features, width, rows), F32),
            pltpu.VMEM((2, NF, width // NF, 2 * width), F32),
            pltpu.VMEM((features // 2, NZ, NX, mine, 2 * width), F32),
            pltpu.VMEM((features, HEADS, rows, 4 * HEAD), BF),
            pltpu.VMEM((features, HEADS // 2, VROWS, rows), BF),
            pltpu.VMEM((features, HEADS, 4 * HEAD, all_tests), BF),
            pltpu.VMEM((2 * width, 4 * width), BF),
            pltpu.VMEM((width, 4 * width), BF),
            pltpu.VMEM((2, width, width), BF),
            pltpu.VMEM((lanes(max(GROUPS)), all_tests), F32),
            pltpu.VMEM((2, 2 * width, rows), F32),
            pltpu.VMEM((HEADS // 2, 2, rows, all_tests), F32),
            dma((features,)),
            dma((2,)),
            dma((2,)),
            dma((features // 2, 6)),
            dma((features // 2, 6)),
            dma((len(GROUPS),)),
            dma((len(GROUPS), 10)),
            [pltpu.VMEM((NZ, NX, mine, lanes(n)), F32) for n in GROUPS],
            inboxes,
            pltpu.VMEM((features, mine, width), F32),
            pltpu.VMEM((4, width // NF, width), F32),
            dma((5,)),
        ],
        compiler_params=pltpu.CompilerParams(
            collective_id=0, has_side_effects=True, vmem_limit_bytes=60 * 2**20
        ),
        name="attention",
    )(cells, tests, w_query, w_key, w_value, w_out)
    return jnp.transpose(out, (1, 0, 2))


def solution(mesh):
    rows = P("rows", "feat", None)
    weights = P("feat", None)
    return jax.shard_map(
        per_device,
        mesh=mesh,
        in_specs=(rows, rows, weights, weights, weights, weights),
        out_specs=rows,
        check_vma=False,
    )
```
